128 devices in a mesh: batch: 1, col: 2 (over core), row: 64 (over z, y, x).
Axes of the slice: x: 4, y: 4, z: 4, core: 2. Of those that a mesh axis runs over, the one named last changes fastest.
Arguments:
- images: bfloat16 [16, 512, 128, 128], P('batch', 'row', 'col')
- w_down1: bfloat16 [4, 4, 128, 256], replicated
- b_down1: float32 [256], replicated
- w_conv1: bfloat16 [3, 3, 256, 256], replicated
- b_conv1: float32 [256], replicated
- w_down2: bfloat16 [4, 4, 256, 256], replicated
- b_down2: float32 [256], replicated
- w_conv2: bfloat16 [3, 3, 256, 256], replicated
- b_conv2: float32 [256], replicated
- w_down3: bfloat16 [4, 4, 256, 256], replicated
- b_down3: float32 [256], replicated
- w_conv3: bfloat16 [3, 3, 256, 256], replicated
- b_conv3: float32 [256], replicated
Outputs:
- output: bfloat16 [16, 64, 16, 256], P('batch', 'row', 'col')
All inputs are finite; a program needn't handle non-finite values.
Results may differ from the reference program's by a relative error of at most 0.00829362.
Values are sent between devices in bfloat16 or wider.
A program may use at most 1 GiB of HBM per device.

```python
import jax
import jax.numpy as jnp
from jax import lax

NUM_IMAGES = 16
IMG_HEIGHT = 512
IMG_WIDTH = 128
CH_IN = 128
CH_ONE = 256
CH_TWO = 256
CH_THREE = 256


def setup_inputs(seed: int = 0, part: int = 0) -> dict:
    key_list = jax.random.split(jax.random.key(seed), 13)
    image_key = jax.random.fold_in(key_list[0], part)
    images = jax.random.normal(image_key, (NUM_IMAGES, IMG_HEIGHT, IMG_WIDTH, CH_IN), jnp.float32)
    drawn_args = {'images': images.astype(jnp.bfloat16)}
    widths = [CH_IN, CH_ONE, CH_TWO, CH_THREE]
    for stage_idx in range(3):
        c_in = widths[stage_idx]
        c_out = widths[stage_idx + 1]
        key_base = 1 + 4 * stage_idx
        w_down = jax.random.normal(key_list[key_base], (4, 4, c_in, c_out), jnp.float32) * (2.0 / (16 * c_in)) ** 0.5
        b_down = 0.25 * jax.random.normal(key_list[key_base + 1], (c_out,), jnp.float32)
        w_conv = jax.random.normal(key_list[key_base + 2], (3, 3, c_out, c_out), jnp.float32) * (2.0 / (9 * c_out)) ** 0.5
        b_conv = 0.25 * jax.random.normal(key_list[key_base + 3], (c_out,), jnp.float32)
        suffix = str(stage_idx + 1)
        drawn_args['w_down' + suffix] = w_down.astype(jnp.bfloat16)
        drawn_args['b_down' + suffix] = b_down
        drawn_args['w_conv' + suffix] = w_conv.astype(jnp.bfloat16)
        drawn_args['b_conv' + suffix] = b_conv
    return drawn_args


def conv_relu(act_in, weight, bias_vec, stride):
    summed = lax.conv_general_dilated(act_in.astype(jnp.float32), weight.astype(jnp.float32), (stride, stride), ((1, 1), (1, 1)), dimension_numbers=('NHWC', 'HWIO', 'NHWC'))
    return jax.nn.relu(summed + bias_vec).astype(jnp.bfloat16)


def reference(images, w_down1, b_down1, w_conv1, b_conv1, w_down2, b_down2, w_conv2, b_conv2, w_down3, b_down3, w_conv3, b_conv3):
    params = [(w_down1, b_down1, w_conv1, b_conv1), (w_down2, b_down2, w_conv2, b_conv2), (w_down3, b_down3, w_conv3, b_conv3)]

    def encode(one_image):
        act_tile = one_image[None]
        for w_down, b_down, w_conv, b_conv in params:
            act_tile = conv_relu(act_tile, w_down, b_down, 2)
            act_tile = conv_relu(act_tile, w_conv, b_conv, 1)
        return act_tile[0]

    return lax.map(encode, images)
```

```python
import functools

import jax
import jax.numpy as jnp
from jax import lax
from jax.experimental import pallas as pl
from jax.experimental.pallas import tpu as pltpu
from jax.sharding import PartitionSpec as P

MESH = pl.DeviceIdType.MESH
LANES = 128
PAD = 8

GROUP = (2, 2, 4, 4, 8, 8)
CHUNK = (1, 1, 4, 4, 8, 8)


def plan(images, rows, width, c_in, c_out):
    layers = []
    for stage in range(3):
        for stride, taps in ((2, 4), (1, 3)):
            layers.append(
                dict(stride=stride, taps=taps, rows=rows, width=width, chan=c_in, out_rows=rows // stride, out_width=width // stride)
            )
            rows, width, c_in = rows // stride, width // stride, c_out
    for i, layer in enumerate(layers):
        layer["group"] = min(GROUP[i], images)
        layer["chunk"] = min(CHUNK[i], images)
        layer["groups"] = images // layer["group"]
    return layers


def kernel(layers, half, row_len, *refs):
    images_ref = refs[0]
    w_hbm, b_hbm = refs[1:13:2], refs[2:14:2]
    out_ref = refs[13]
    refs = refs[14:]
    ximg, xhalo, feat = refs[:3]
    w_refs, b_refs = refs[3:9], refs[9:15]
    a_refs = refs[15:21]
    s_refs = refs[21:27]
    send_bufs, halo_bufs = refs[27:32], refs[32:37]
    w_sem, b_sem, own_sem, part_send, part_recv, edge_send, edge_recv, out_sem = refs[37:45]
    y_send, y_recv = refs[45:50], refs[50:55]

    k = lax.axis_index("col")
    row = lax.axis_index("row")
    has = (row > 0, row < row_len - 1)
    near = (jnp.maximum(row - 1, 0), jnp.minimum(row + 1, row_len - 1))
    col_half = layers[0]["width"] // 2
    last_row = layers[0]["rows"] - 1

    barrier = pltpu.get_barrier_semaphore()
    pl.semaphore_signal(barrier, inc=1, device_id={"col": 1 - k}, device_id_type=MESH)
    for d in range(2):
        @pl.when(has[d])
        def _():
            for c in range(2):
                pl.semaphore_signal(barrier, inc=1, device_id={"col": c, "row": near[d]}, device_id_type=MESH)

    g0, n_groups0 = layers[0]["group"], layers[0]["groups"]

    def own_copy(g):
        src = images_ref.at[pl.ds(k * half + g * g0, g0)]
        return pltpu.make_async_copy(src, ximg.at[k, pl.ds(g * g0, g0)], own_sem.at[g])

    def part_copy(g):
        src = images_ref.at[pl.ds((1 - k) * half + g * g0, g0)]
        return pltpu.make_async_remote_copy(
            src, ximg.at[k, pl.ds(g * g0, g0)], part_send.at[g], part_recv.at[g], device_id={"col": 1 - k}, device_id_type=MESH
        )

    def part_arrival(g):
        dst = ximg.at[1 - k, pl.ds(g * g0, g0)]
        return pltpu.make_async_remote_copy(
            dst, dst, part_send.at[g], part_recv.at[g], device_id={"col": 1 - k}, device_id_type=MESH
        )

    def edge_copy(d, c, g):
        src = images_ref.at[pl.ds(c * half + g * g0, g0), 0 if d == 0 else last_row]
        return pltpu.make_async_remote_copy(
            src,
            xhalo.at[1 - d, k, pl.ds(g * g0, g0)],
            edge_send.at[d, c, g],
            edge_recv.at[1 - d, k, g],
            device_id={"col": c, "row": near[d]},
            device_id_type=MESH,
        )

    def edge_arrival(d, c, g):
        dst = xhalo.at[d, c, pl.ds(g * g0, g0)]
        return pltpu.make_async_remote_copy(
            dst, dst, edge_send.at[d, c, g], edge_recv.at[d, c, g], device_id={"col": c, "row": near[d]}, device_id_type=MESH
        )

    def y_copy(i, d, g):
        n = layers[i]["group"]
        return pltpu.make_async_remote_copy(
            send_bufs[i].at[d, pl.ds(g * n, n)],
            halo_bufs[i].at[1 - d, pl.ds(g * n, n)],
            y_send[i].at[d, g],
            y_recv[i].at[1 - d, g],
            device_id={"row": near[d]},
            device_id_type=MESH,
        )

    def y_arrival(i, d, g):
        n = layers[i]["group"]
        dst = halo_bufs[i].at[d, pl.ds(g * n, n)]
        return pltpu.make_async_remote_copy(
            dst, dst, y_send[i].at[d, g], y_recv[i].at[d, g], device_id={"row": near[d]}, device_id_type=MESH
        )

    def w_copy(i):
        return pltpu.make_async_copy(w_hbm[i], w_refs[i], w_sem.at[i])

    def b_copy(i):
        return pltpu.make_async_copy(b_hbm[i], b_refs[i], b_sem.at[i])

    own_copy(0).start()
    w_copy(0).start()
    for g in range(1, n_groups0):
        own_copy(g).start()
    for i in range(6):
        b_copy(i).start()
    for i in range(1, 6):
        w_copy(i).start()

    for i, layer in enumerate(layers):
        w = layer["width"]
        s = s_refs[i]
        edge = jnp.zeros(s.shape[:-2] + (PAD, LANES), jnp.float32)
        s[..., pl.ds(0, PAD), :] = edge
        s[..., pl.ds(PAD + w, PAD), :] = edge
    for d in range(2):
        @pl.when(jnp.logical_not(has[d]))
        def _():
            xhalo[d] = jnp.zeros(xhalo.shape[1:], xhalo.dtype)
            for h in halo_bufs:
                h[d] = jnp.zeros(h.shape[1:], h.dtype)

    pl.semaphore_wait(barrier, 1 + 2 * (has[0].astype(jnp.int32) + has[1].astype(jnp.int32)))

    for g in range(n_groups0):
        for d in range(2):
            @pl.when(has[d])
            def _():
                for c in range(2):
                    edge_copy(d, c, g).start()
        part_copy(g).start()

    def taps_from(i, slot, img, first, count):
        layer = layers[i]
        s, a = s_refs[i], a_refs[i]
        chan, w, stride = layer["chan"], layer["out_width"], layer["stride"]
        for q in range(layer["taps"]):
            for h in range(chan // LANES):
                lanes = pl.ds(q * chan + h * LANES, LANES)
                for r in range(first, first + count):
                    at = pl.ds(PAD - 1 + q, w) if stride == 1 else pl.ds(PAD - 1 + q, w, stride=2)
                    v = s[slot, h, r, at, :].astype(jnp.bfloat16)
                    if stride == 1:
                        a[img, r, :, lanes] = v
                    else:
                        a[img, r % 2, r // 2, :, lanes] = v

    def layer_step(i, g):
        layer = layers[i]
        n, chunk, rows, w = layer["group"], layer["chunk"], layer["rows"], layer["width"]
        out_rows, out_w, taps = layer["out_rows"], layer["out_width"], layer["taps"]
        s, a = s_refs[i], a_refs[i]
        base = g * n
        if i == 0:
            own_copy(g).wait()
            part_arrival(g).wait_recv()
            for d in range(2):
                @pl.when(has[d])
                def _():
                    for c in range(2):
                        edge_arrival(d, c, g).wait_recv()
        else:
            before = layers[i - 1]["group"]
            for d in range(2):
                @pl.when(has[d])
                def _():
                    for j in range(n // before):
                        y_arrival(i - 1, d, g * (n // before) + j).wait_recv()

        for m in range(0, n, chunk):
            imgs = [base + m + j for j in range(chunk)]
            for j, img in enumerate(imgs):
                slot = m + j
                if i == 0:
                    for c in range(2):
                        at = pl.ds(PAD + c * col_half, col_half)
                        s[slot, 0, 0, at, :] = xhalo[0, c, img].astype(jnp.float32)
                        s[slot, 0, pl.ds(1, rows), at, :] = ximg[c, img].astype(jnp.float32)
                        s[slot, 0, rows + 1, at, :] = xhalo[1, c, img].astype(jnp.float32)
                    taps_from(i, slot, slot, 0, rows + 2)
                else:
                    for d, r in ((0, 0), (1, rows + 1)):
                        v = halo_bufs[i - 1][d, img].astype(jnp.float32)
                        for h in range(layer["chan"] // LANES):
                            s[slot, h, r, pl.ds(PAD, w), :] = v[:, h * LANES : (h + 1) * LANES]
                        taps_from(i, slot, img, r, 1)
            size = chunk * out_rows * out_w
            first = m if i == 0 else base + m
            acc = None
            for p in range(taps):
                if layer["stride"] == 1:
                    left = a[pl.ds(first, chunk), pl.ds(p, out_rows)]
                else:
                    left = a[pl.ds(first, chunk), p % 2, pl.ds(p // 2, out_rows)]
                part = jnp.dot(left.reshape(size, left.shape[-1]), w_refs[i][p], preferred_element_type=jnp.float32)
                acc = part if acc is None else acc + part
            v = jnp.maximum(acc + b_refs[i][...], 0.0)
            c_out = v.shape[-1]
            if i == 5:
                v = v.reshape(chunk, out_w, c_out)
                for c in range(2):
                    feat[c, pl.ds(base + m, chunk)] = v[:, c * out_w // 2 : (c + 1) * out_w // 2].astype(jnp.bfloat16)
                continue
            v = v.reshape(chunk, out_rows, out_w, c_out)
            for d, r in ((0, 0), (1, out_rows - 1)):
                send_bufs[i][d, pl.ds(base + m, chunk)] = v[:, r].astype(jnp.bfloat16)
            nxt = s_refs[i + 1]
            slots = nxt.shape[0]
            for j, img in enumerate(imgs):
                slot = (m + j) % slots
                for h in range(c_out // LANES):
                    nxt[slot, h, pl.ds(1, out_rows), pl.ds(PAD, out_w), :] = v[j, :, :, h * LANES : (h + 1) * LANES]
                taps_from(i + 1, slot, img, 1, out_rows)
        if i < 5:
            for d in range(2):
                @pl.when(has[d])
                def _():
                    y_copy(i, d, g).start()

    for i in range(6):
        w_copy(i).wait()
        b_copy(i).wait()
        if layers[i]["groups"] == 1:
            layer_step(i, 0)
        else:
            @pl.loop(0, layers[i]["groups"])
            def _(g):
                layer_step(i, g)

    mine = pltpu.make_async_copy(feat.at[k], out_ref.at[pl.ds(k * half, half), 0], out_sem.at[0])
    theirs = pltpu.make_async_remote_copy(
        feat.at[1 - k],
        out_ref.at[pl.ds(k * half, half), 0],
        out_sem.at[1],
        out_sem.at[2],
        device_id={"col": 1 - k},
        device_id_type=MESH,
    )
    arriving = pltpu.make_async_remote_copy(
        feat.at[1 - k],
        out_ref.at[pl.ds((1 - k) * half, half), 0],
        out_sem.at[1],
        out_sem.at[2],
        device_id={"col": 1 - k},
        device_id_type=MESH,
    )
    theirs.start()
    mine.start()

    for g in range(n_groups0):
        part_copy(g).wait_send()
        for d in range(2):
            @pl.when(has[d])
            def _():
                for c in range(2):
                    edge_copy(d, c, g).wait_send()
    for i in range(5):
        for g in range(layers[i]["groups"]):
            for d in range(2):
                @pl.when(has[d])
                def _():
                    y_copy(i, d, g).wait_send()
    mine.wait()
    theirs.wait_send()
    arriving.wait_recv()


def solution(mesh):
    row_len = mesh.shape["row"]

    def local_encoder(images, *params):
        n_img, rows, col_half, c_in = images.shape
        half = n_img // 2
        weights, biases = params[0::2], params[1::2]
        c_out = weights[0].shape[-1]
        layers = plan(half, rows, 2 * col_half, c_in, c_out)
        args = [images]
        for w, b in zip(weights, biases):
            args += [w.reshape(w.shape[0], w.shape[1] * w.shape[2], c_out), b.reshape(1, c_out)]

        bf16, f32 = jnp.bfloat16, jnp.float32
        scratch = [
            pltpu.VMEM((2, half, rows, col_half, c_in), bf16),
            pltpu.VMEM((2, 2, half, col_half, c_in), bf16),
            pltpu.VMEM((2, half, layers[5]["out_width"] // 2, c_out), bf16),
        ]
        scratch += [pltpu.VMEM(w.shape, bf16) for w in args[1::2]]
        scratch += [pltpu.VMEM((1, c_out), f32) for _ in biases]
        for i, la in enumerate(layers):
            held = la["group"] if i == 0 else half
            depth = la["taps"] * la["chan"]
            if la["stride"] == 1:
                shape = (held, la["rows"] + 2, la["out_width"], depth)
            else:
                shape = (held, 2, (la["rows"] + 2) // 2, la["out_width"], depth)
            scratch.append(pltpu.VMEM(shape, bf16))
        for la in layers:
            scratch.append(pltpu.VMEM((la["group"], la["chan"] // LANES, la["rows"] + 2, la["width"] + 3 * PAD, LANES), f32))
        edges = [pltpu.VMEM((2, half, la["out_width"], c_out), bf16) for la in layers[:5]]
        scratch += edges + edges
        dma = pltpu.SemaphoreType.DMA
        g0 = layers[0]["groups"]
        scratch += [dma((6,)), dma((6,)), dma((g0,)), dma((g0,)), dma((g0,)), dma((2, 2, g0)), dma((2, 2, g0)), dma((3,))]
        sems = [dma((2, la["groups"])) for la in layers[:5]]
        scratch += sems + sems

        any_spec = pl.BlockSpec(memory_space=pl.ANY)
        return pl.pallas_call(
            functools.partial(kernel, layers, half, row_len),
            out_shape=jax.ShapeDtypeStruct((n_img, rows // 8, col_half // 8, c_out), bf16),
            in_specs=[any_spec] * len(args),
            out_specs=any_spec,
            scratch_shapes=scratch,
            compiler_params=pltpu.CompilerParams(collective_id=0, has_side_effects=True, vmem_limit_bytes=60 * 1024 * 1024),
            name="encoder",
        )(*args)

    tile_spec = P("batch", "row", "col", None)
    return jax.shard_map(local_encoder, mesh=mesh, in_specs=(tile_spec,) + (P(),) * 12, out_specs=tile_spec, check_vma=False)
```

```python
import functools

import jax
import jax.numpy as jnp
from jax import lax
from jax.experimental import pallas as pl
from jax.experimental.pallas import tpu as pltpu
from jax.sharding import PartitionSpec as P

MESH = pl.DeviceIdType.MESH
LANES = 128
PAD = 8

GROUP = (1, 1, 2, 2, 4)
PHASES = ((0,), (1,), (2,), (3, 4), (5,))
EXT_IN = (1, 1, 1, 2, 1, 1)
EXT_OUT = (0, 0, 0, 1, 0, 0)
LAST = len(PHASES) - 1


def plan(images, rows, width, c_in, c_out):
    layers = []
    for i in range(6):
        stride, taps = ((2, 4), (1, 3))[i % 2]
        phase = [p for p in range(len(PHASES)) if i in PHASES[p]][0]
        layers.append(
            dict(
                stride=stride, taps=taps, rows=rows, width=width, chan=c_in, out_rows=rows // stride, out_width=width // stride,
                ext=EXT_IN[i], ext_out=EXT_OUT[i], group=min(GROUP[phase], images),
            )
        )
        rows, width, c_in = rows // stride, width // stride, c_out
    return layers


def kernel(layers, half, row_len, *refs):
    images_ref = refs[0]
    w_hbm, b_hbm = refs[1:13:2], refs[2:14:2]
    out_ref = refs[13]
    refs = refs[14:]
    ximg, xedge, xhalo, feat = refs[:4]
    w_refs, b_refs = refs[4:10], refs[10:16]
    a_refs = refs[16:22]
    s_refs = refs[22:28]
    refs = refs[28:]
    send_bufs, halo_bufs = refs[:LAST], refs[LAST : 2 * LAST]
    refs = refs[2 * LAST :]
    w_sem, b_sem, own_sem, part_send, part_recv, load_sem, edge_send, edge_recv, out_sem = refs[:9]
    y_send, y_recv = refs[9 : 9 + LAST], refs[9 + LAST :]

    k = lax.axis_index("col")
    row = lax.axis_index("row")
    has = (row > 0, row < row_len - 1)
    near = (jnp.maximum(row - 1, 0), jnp.minimum(row + 1, row_len - 1))
    col_half = layers[0]["width"] // 2
    last_row = layers[0]["rows"] - 1
    g0 = layers[0]["group"]
    n_groups0 = half // g0

    barrier = pltpu.get_barrier_semaphore()
    for d in range(2):
        @pl.when(has[d])
        def _():
            for c in range(2):
                pl.semaphore_signal(barrier, inc=1, device_id={"col": c, "row": near[d]}, device_id_type=MESH)
    pl.semaphore_signal(barrier, inc=1, device_id={"col": 1 - k}, device_id_type=MESH)

    def edge_load(d):
        return pltpu.make_async_copy(images_ref.at[:, 0 if d == 0 else last_row], xedge.at[d], load_sem.at[d])

    def own_copy(g):
        src = images_ref.at[pl.ds(k * half + g * g0, g0)]
        return pltpu.make_async_copy(src, ximg.at[k, pl.ds(g * g0, g0)], own_sem.at[g])

    def part_copy(g):
        src = images_ref.at[pl.ds((1 - k) * half + g * g0, g0)]
        return pltpu.make_async_remote_copy(
            src, ximg.at[k, pl.ds(g * g0, g0)], part_send.at[g], part_recv.at[g], device_id={"col": 1 - k}, device_id_type=MESH
        )

    def part_arrival(g):
        dst = ximg.at[1 - k, pl.ds(g * g0, g0)]
        return pltpu.make_async_remote_copy(
            dst, dst, part_send.at[g], part_recv.at[g], device_id={"col": 1 - k}, device_id_type=MESH
        )

    def edge_copy(d, c, g):
        return pltpu.make_async_remote_copy(
            xedge.at[d, pl.ds(c * half + g * g0, g0)],
            xhalo.at[1 - d, k, pl.ds(g * g0, g0)],
            edge_send.at[d, c, g],
            edge_recv.at[1 - d, k, g],
            device_id={"col": c, "row": near[d]},
            device_id_type=MESH,
        )

    def edge_arrival(d, c, g):
        dst = xhalo.at[d, c, pl.ds(g * g0, g0)]
        return pltpu.make_async_remote_copy(
            dst, dst, edge_send.at[d, c, g], edge_recv.at[d, c, g], device_id={"col": c, "row": near[d]}, device_id_type=MESH
        )

    def y_copy(x, d, g):
        n = layers[PHASES[x][0]]["group"]
        return pltpu.make_async_remote_copy(
            send_bufs[x].at[d, pl.ds(g * n, n)],
            halo_bufs[x].at[1 - d, pl.ds(g * n, n)],
            y_send[x].at[d, g],
            y_recv[x].at[1 - d, g],
            device_id={"row": near[d]},
            device_id_type=MESH,
        )

    def y_arrival(x, d, g):
        n = layers[PHASES[x][0]]["group"]
        dst = halo_bufs[x].at[d, pl.ds(g * n, n)]
        return pltpu.make_async_remote_copy(
            dst, dst, y_send[x].at[d, g], y_recv[x].at[d, g], device_id={"row": near[d]}, device_id_type=MESH
        )

    def w_copy(i):
        return pltpu.make_async_copy(w_hbm[i], w_refs[i], w_sem.at[i])

    def b_copy(i):
        return pltpu.make_async_copy(b_hbm[i], b_refs[i], b_sem.at[i])

    for d in range(2):
        edge_load(d).start()
    own_copy(0).start()
    w_copy(0).start()
    for g in range(1, n_groups0):
        own_copy(g).start()
    for i in range(6):
        b_copy(i).start()

    for d in range(2):
        edge_load(d).wait()
    pl.semaphore_wait(barrier, 1 + 2 * (has[0].astype(jnp.int32) + has[1].astype(jnp.int32)))

    for g in range(n_groups0):
        for d in range(2):
            @pl.when(has[d])
            def _():
                for c in range(2):
                    edge_copy(d, c, g).start()
        part_copy(g).start()
    for i in range(1, 6):
        w_copy(i).start()

    for i, layer in enumerate(layers):
        w = layer["width"]
        s = s_refs[i]
        edge = jnp.zeros(s.shape[:-2] + (PAD, LANES), jnp.float32)
        s[..., pl.ds(0, PAD), :] = edge
        s[..., pl.ds(PAD + w, PAD), :] = edge
    for d in range(2):
        @pl.when(jnp.logical_not(has[d]))
        def _():
            xhalo[d] = jnp.zeros(xhalo.shape[1:], xhalo.dtype)
            for h in halo_bufs:
                h[d] = jnp.zeros(h.shape[1:], h.dtype)

    def taps_from(i, slot, img, rows):
        layer = layers[i]
        s, a = s_refs[i], a_refs[i]
        chan, w, stride = layer["chan"], layer["out_width"], layer["stride"]
        tiles = [(q, h) for q in range(layer["taps"]) for h in range(chan // LANES)]
        for r in rows:
            for t in range(0, len(tiles), 2):
                pair = []
                for q, h in tiles[t : t + 2]:
                    at = pl.ds(PAD - 1 + q, w) if stride == 1 else pl.ds(PAD - 1 + q, w, stride=2)
                    pair.append(s[slot, h, r, at, :])
                v = jnp.concatenate(pair, axis=-1).astype(jnp.bfloat16)
                lanes = pl.ds(t * LANES, 2 * LANES)
                if stride == 1:
                    a[img, r, :, lanes] = v
                else:
                    a[img, r % 2, r // 2, :, lanes] = v

    def product(i, first, chunk):
        layer = layers[i]
        a, out_rows = a_refs[i], layer["out_rows"] + 2 * layer["ext_out"]
        acc = None
        for p in range(layer["taps"]):
            if layer["stride"] == 1:
                left = a[pl.ds(first, chunk), pl.ds(p, out_rows)]
            else:
                left = a[pl.ds(first, chunk), p % 2, pl.ds(p // 2, out_rows)]
            left = left.reshape(chunk * out_rows * layer["out_width"], left.shape[-1])
            part = jnp.dot(left, w_refs[i][p], preferred_element_type=jnp.float32)
            acc = part if acc is None else acc + part
        v = jnp.maximum(acc + b_refs[i][...], 0.0)
        return v.reshape(chunk, out_rows, layer["out_width"], v.shape[-1])

    def keep_rows(i, slot, v, r):
        w = layers[i]["width"]
        for h in range(v.shape[-1] // LANES):
            s_refs[i][slot, h, pl.ds(r, v.shape[0]), pl.ds(PAD, w), :] = v[:, :, h * LANES : (h + 1) * LANES]

    def phase_step(phase, g):
        first = layers[PHASES[phase][0]]
        n = first["group"]
        base = g * n
        if phase == 0:
            own_copy(g).wait()
            part_arrival(g).wait_recv()
            for d in range(2):
                @pl.when(has[d])
                def _():
                    for c in range(2):
                        edge_arrival(d, c, g).wait_recv()
        else:
            before = layers[PHASES[phase - 1][0]]["group"]
            for d in range(2):
                @pl.when(has[d])
                def _():
                    for j in range(n // before):
                        y_arrival(phase - 1, d, g * (n // before) + j).wait_recv()

        for j in range(n):
            img = base + j
            if phase == 0:
                rows = first["rows"]
                for c in range(2):
                    at = pl.ds(PAD + c * col_half, col_half)
                    s = s_refs[0]
                    s[j, 0, 0, at, :] = xhalo[0, c, img].astype(jnp.float32)
                    s[j, 0, pl.ds(1, rows), at, :] = ximg[c, img].astype(jnp.float32)
                    s[j, 0, rows + 1, at, :] = xhalo[1, c, img].astype(jnp.float32)
                taps_from(0, j, j, range(rows + 2))
            else:
                i, ext = PHASES[phase][0], first["ext"]
                for d, r in ((0, 0), (1, first["rows"] + ext)):
                    keep_rows(i, j, halo_bufs[phase - 1][d, img].astype(jnp.float32), r)
                    taps_from(i, j, img, range(r, r + ext))

        for i in PHASES[phase]:
            layer = layers[i]
            local = i != PHASES[phase][0] or i == 0
            chunk = n if i >= 2 else 1
            for m in range(0, n, chunk):
                v = product(i, m if local else base + m, chunk)
                if i == 5:
                    w = layer["out_width"]
                    for c in range(2):
                        feat[c, pl.ds(base + m, chunk)] = v[:, 0, c * w // 2 : (c + 1) * w // 2].astype(jnp.bfloat16)
                    continue
                ext, out_rows = layer["ext_out"], layer["out_rows"]
                if i == PHASES[phase][-1]:
                    x = phase
                    depth = send_bufs[x].shape[2]
                    for d, r in ((0, 0), (1, out_rows - depth)):
                        send_bufs[x][d, pl.ds(base + m, chunk)] = v[:, r : r + depth].astype(jnp.bfloat16)
                    slots = s_refs[i + 1].shape[0]
                    r0 = layers[i + 1]["ext"]
                    for j in range(chunk):
                        slot = (m + j) % slots
                        keep_rows(i + 1, slot, v[j], r0)
                        taps_from(i + 1, slot, base + m + j, range(r0, r0 + out_rows))
                else:
                    for j in range(chunk):
                        slot = m + j
                        keep_rows(i + 1, slot, jnp.where(has[0], v[j, :ext], 0.0), 0)
                        keep_rows(i + 1, slot, v[j, ext : ext + out_rows], ext)
                        keep_rows(i + 1, slot, jnp.where(has[1], v[j, ext + out_rows :], 0.0), ext + out_rows)
                        taps_from(i + 1, slot, slot, range(out_rows + 2 * ext))
        if phase < LAST:
            for d in range(2):
                @pl.when(has[d])
                def _():
                    y_copy(phase, d, g).start()

    for phase in range(LAST + 1):
        for i in PHASES[phase]:
            w_copy(i).wait()
            b_copy(i).wait()
        groups = half // layers[PHASES[phase][0]]["group"]
        if groups == 1:
            phase_step(phase, 0)
        else:
            @pl.loop(0, groups)
            def _(g):
                phase_step(phase, g)

    mine = pltpu.make_async_copy(feat.at[k], out_ref.at[pl.ds(k * half, half), 0], out_sem.at[0])
    theirs = pltpu.make_async_remote_copy(
        feat.at[1 - k],
        out_ref.at[pl.ds(k * half, half), 0],
        out_sem.at[1],
        out_sem.at[2],
        device_id={"col": 1 - k},
        device_id_type=MESH,
    )
    arriving = pltpu.make_async_remote_copy(
        feat.at[1 - k],
        out_ref.at[pl.ds((1 - k) * half, half), 0],
        out_sem.at[1],
        out_sem.at[2],
        device_id={"col": 1 - k},
        device_id_type=MESH,
    )
    theirs.start()
    mine.start()

    for g in range(n_groups0):
        part_copy(g).wait_send()
        for d in range(2):
            @pl.when(has[d])
            def _():
                for c in range(2):
                    edge_copy(d, c, g).wait_send()
    for x in range(LAST):
        for g in range(half // layers[PHASES[x][0]]["group"]):
            for d in range(2):
                @pl.when(has[d])
                def _():
                    y_copy(x, d, g).wait_send()
    mine.wait()
    theirs.wait_send()
    arriving.wait_recv()


def solution(mesh):
    row_len = mesh.shape["row"]

    def local_encoder(images, *params):
        n_img, rows, col_half, c_in = images.shape
        half = n_img // 2
        weights, biases = params[0::2], params[1::2]
        c_out = weights[0].shape[-1]
        layers = plan(half, rows, 2 * col_half, c_in, c_out)
        args = [images]
        for w, b in zip(weights, biases):
            args += [w.reshape(w.shape[0], w.shape[1] * w.shape[2], c_out), b.reshape(1, c_out)]

        bf16, f32 = jnp.bfloat16, jnp.float32
        scratch = [
            pltpu.VMEM((2, half, rows, col_half, c_in), bf16),
            pltpu.VMEM((2, n_img, col_half, c_in), bf16),
            pltpu.VMEM((2, 2, half, col_half, c_in), bf16),
            pltpu.VMEM((2, half, layers[5]["out_width"] // 2, c_out), bf16),
        ]
        scratch += [pltpu.VMEM(w.shape, bf16) for w in args[1::2]]
        scratch += [pltpu.VMEM((1, c_out), f32) for _ in biases]
        for i, la in enumerate(layers):
            held = half if i in [p[0] for p in PHASES[1:]] else la["group"]
            depth = la["taps"] * la["chan"]
            total = la["rows"] + 2 * la["ext"]
            if la["stride"] == 1:
                shape = (held, total, la["out_width"], depth)
            else:
                shape = (held, 2, total // 2, la["out_width"], depth)
            scratch.append(pltpu.VMEM(shape, bf16))
        for la in layers:
            total = la["rows"] + 2 * la["ext"]
            scratch.append(pltpu.VMEM((la["group"], la["chan"] // LANES, total, la["width"] + 3 * PAD, LANES), f32))
        edges = [pltpu.VMEM((2, half, layers[i]["ext"], layers[i]["width"], c_out), bf16) for i in [p[0] for p in PHASES[1:]]]
        scratch += edges + edges
        dma = pltpu.SemaphoreType.DMA
        g0 = half // layers[0]["group"]
        scratch += [dma((6,)), dma((6,)), dma((g0,)), dma((g0,)), dma((g0,)), dma((2,)), dma((2, 2, g0)), dma((2, 2, g0)), dma((3,))]
        sems = [dma((2, half // layers[i]["group"])) for i in [p[0] for p in PHASES[:-1]]]
        scratch += sems + sems

        any_spec = pl.BlockSpec(memory_space=pl.ANY)
        return pl.pallas_call(
            functools.partial(kernel, layers, half, row_len),
            out_shape=jax.ShapeDtypeStruct((n_img, rows // 8, col_half // 8, c_out), bf16),
            in_specs=[any_spec] * len(args),
            out_specs=any_spec,
            scratch_shapes=scratch,
            compiler_params=pltpu.CompilerParams(collective_id=0, has_side_effects=True, vmem_limit_bytes=60 * 1024 * 1024),
            name="encoder",
        )(*args)

    tile_spec = P("batch", "row", "col", None)
    return jax.shard_map(local_encoder, mesh=mesh, in_specs=(tile_spec,) + (P(),) * 12, out_specs=tile_spec, check_vma=False)
```

```python
import functools

import jax
import jax.numpy as jnp
from jax import lax
from jax.experimental import pallas as pl
from jax.experimental.pallas import tpu as pltpu
from jax.sharding import PartitionSpec as P

MESH = pl.DeviceIdType.MESH
LANES = 128
PAD = 8
RING = 4

LAYERS = ((2, 4, 1), (1, 3, 2), (2, 4, 1), (1, 3, 4), (2, 4, 3), (1, 3, 1))
BF16, F32 = jnp.bfloat16, jnp.float32


def kernel(half, row_len, *refs):
    images_ref = refs[0]
    w_hbm, b_hbm = refs[1:13:2], refs[2:14:2]
    out_ref = refs[13]
    refs = refs[14:]
    ximg, xedge, xhalo, y_out, y_in, y_halo, u_out, u_halo, f_out, f_in = refs[:10]
    w_refs, b_refs, a_refs, s_refs = refs[10:16], refs[16:22], refs[22:28], refs[28:34]
    (w_sem, b_sem, own_sem, part_send, part_recv, load_sem, edge_send, edge_recv) = refs[34:42]
    (y_send, y_recv, yh_send, yh_recv, u_send, u_recv, f_send, f_recv) = refs[42:]

    k = lax.axis_index("col")
    row = lax.axis_index("row")
    x = row % RING
    first = row - x
    per = half // RING
    has = (row > 0, row < row_len - 1)
    near = (jnp.maximum(row - 1, 0), jnp.minimum(row + 1, row_len - 1))
    has_block = (row >= RING, row < row_len - RING)
    near_block = (jnp.maximum(row - RING, 0), jnp.minimum(row + RING, row_len - 1))
    tile_rows = ximg.shape[2]
    col_half = ximg.shape[3]
    y_part = y_out.shape[2]
    y_rows = 2 * y_part

    barrier = pltpu.get_barrier_semaphore()
    crosses = (jnp.logical_and(has[0], x == 0), jnp.logical_and(has[1], x == RING - 1))
    for d in range(2):
        @pl.when(crosses[d])
        def _():
            for c in range(2):
                pl.semaphore_signal(barrier, inc=1, device_id={"col": c, "row": near[d]}, device_id_type=MESH)

        @pl.when(has_block[d])
        def _():
            pl.semaphore_signal(barrier, inc=1, device_id={"row": near_block[d]}, device_id_type=MESH)
    for o in (2, 1, 3):
        for c in range(2):
            pl.semaphore_signal(barrier, inc=1, device_id={"col": c, "row": first + (x + o) % RING}, device_id_type=MESH)
    pl.semaphore_signal(barrier, inc=1, device_id={"col": 1 - k}, device_id_type=MESH)

    def turn(i, at):
        step, pair = i % RING, (i % RING) // 2
        offset = (1 - pair) * (2 + step) + pair * (3 - step)
        return (i // RING) * RING + (at + offset) % RING

    def edge_load(d):
        return pltpu.make_async_copy(images_ref.at[:, 0 if d == 0 else tile_rows - 1], xedge.at[d], load_sem.at[d])

    def own_copy(j):
        return pltpu.make_async_copy(images_ref.at[k * half + j], ximg.at[k, j], own_sem.at[j])

    def part_copy(j):
        return pltpu.make_async_remote_copy(
            images_ref.at[(1 - k) * half + j], ximg.at[k, j], part_send.at[j], part_recv.at[j],
            device_id={"col": 1 - k}, device_id_type=MESH,
        )

    def part_arrival(j):
        dst = ximg.at[1 - k, j]
        return pltpu.make_async_remote_copy(
            dst, dst, part_send.at[j], part_recv.at[j], device_id={"col": 1 - k}, device_id_type=MESH
        )

    def edge_copy(d, c, j):
        return pltpu.make_async_remote_copy(
            xedge.at[d, c * half + j], xhalo.at[1 - d, k, j], edge_send.at[d, c, j], edge_recv.at[1 - d, k, j],
            device_id={"col": c, "row": near[d]}, device_id_type=MESH,
        )

    def edge_arrival(d, c, j):
        dst = xhalo.at[d, c, j]
        return pltpu.make_async_remote_copy(
            dst, dst, edge_send.at[d, c, j], edge_recv.at[d, c, j], device_id={"col": c, "row": near[d]}, device_id_type=MESH
        )

    def y_copy(j, e):
        return pltpu.make_async_remote_copy(
            y_out.at[j, e], y_in.at[j // RING, x, e], y_send.at[j, e], y_recv.at[j // RING, x, e],
            device_id={"row": first + j % RING}, device_id_type=MESH,
        )

    def y_stays(j, e):
        return pltpu.make_async_copy(y_out.at[j, e], y_in.at[j // RING, x, e], y_recv.at[j // RING, x, e])

    def y_leaves(j, e):
        stays = j % RING == x

        @pl.when(stays)
        def _():
            y_stays(j, e).start()

        @pl.when(jnp.logical_not(stays))
        def _():
            y_copy(j, e).start()

    def y_arrival(r, src, e):
        dst = y_in.at[r, src, e]
        return pltpu.make_async_copy(dst, dst, y_recv.at[r, src, e])

    def block_copy(src, halo, d, r, send, recv):
        return pltpu.make_async_remote_copy(
            src, halo.at[1 - d, r], send.at[d, r], recv.at[1 - d, r], device_id={"row": near_block[d]}, device_id_type=MESH
        )

    def yh_copy(d, r):
        return block_copy(y_in.at[r, d * (RING - 1), d], y_halo, d, r, yh_send, yh_recv)

    def u_copy(d, r):
        return block_copy(u_out.at[d, r], u_halo, d, r, u_send, u_recv)

    def block_arrival(halo, d, r, send, recv):
        dst = halo.at[d, r]
        return pltpu.make_async_remote_copy(
            dst, dst, send.at[d, r], recv.at[d, r], device_id={"row": near_block[d]}, device_id_type=MESH
        )

    def f_copy(o, c):
        to = (x + o) % RING
        return pltpu.make_async_remote_copy(
            f_out.at[to, c], f_in.at[k, x], f_send.at[o, c], f_recv.at[k, x],
            device_id={"col": c, "row": first + to}, device_id_type=MESH,
        )

    def f_stays():
        return pltpu.make_async_copy(f_out.at[x, k], f_in.at[k, x], f_recv.at[k, x])

    def f_arrival(c, src):
        dst = f_in.at[c, src]
        return pltpu.make_async_copy(dst, dst, f_recv.at[c, src])

    def w_copy(i):
        return pltpu.make_async_copy(w_hbm[i], w_refs[i], w_sem.at[i])

    def b_copy(i):
        return pltpu.make_async_copy(b_hbm[i], b_refs[i], b_sem.at[i])

    for d in range(2):
        edge_load(d).start()
    for i in range(half):
        own_copy(turn(i, x)).start()
        if i == 0:
            w_copy(0).start()
    for i in range(6):
        b_copy(i).start()

    for (stride, _, _), s in zip(LAYERS, s_refs):
        w = s.shape[-2] - 3 * PAD
        edge = jnp.zeros(s.shape[:-2] + (PAD, LANES), F32)
        s[..., pl.ds(0, PAD), :] = edge
        s[..., pl.ds(PAD + w, PAD), :] = edge
    for d in range(2):
        @pl.when(jnp.logical_not(has[d]))
        def _():
            xhalo[d] = jnp.zeros(xhalo.shape[1:], BF16)

        @pl.when(jnp.logical_not(has_block[d]))
        def _():
            y_halo[d] = jnp.zeros(y_halo.shape[1:], BF16)
            u_halo[d] = jnp.zeros(u_halo.shape[1:], BF16)

    for d in range(2):
        edge_load(d).wait()
    count = 2 * RING - 1
    for d in range(2):
        count = count + 2 * crosses[d].astype(jnp.int32) + has_block[d].astype(jnp.int32)
    pl.semaphore_wait(barrier, count)

    for i in range(half):
        part_copy(turn(i, x)).start()
        for d in range(2):
            @pl.when(has[d])
            def _():
                for c in range(2):
                    edge_copy(d, c, turn(i, (x + 2 * d - 1) % RING)).start()
    for i in range(1, 6):
        w_copy(i).start()

    def keep(i, v, r):
        s = s_refs[i]
        w = s.shape[-2] - 3 * PAD
        for h in range(v.shape[-1] // LANES):
            s[h, pl.ds(r, v.shape[0]), pl.ds(PAD, w), :] = v[:, :, h * LANES : (h + 1) * LANES]

    def spread(i, rows, a):
        stride, taps, _ = LAYERS[i]
        s = s_refs[i]
        w = (s.shape[-2] - 3 * PAD) // stride
        tiles = [(q, h) for q in range(taps) for h in range(s.shape[0])]
        for r in rows:
            for t in range(0, len(tiles), 2):
                pair = []
                for q, h in tiles[t : t + 2]:
                    at = pl.ds(PAD - 1 + q, w) if stride == 1 else pl.ds(PAD - 1 + q, w, stride=2)
                    pair.append(s[h, r, at, :])
                v = jnp.concatenate(pair, axis=-1).astype(BF16)
                lanes = pl.ds(t * LANES, 2 * LANES)
                if stride == 1:
                    a[r, :, lanes] = v
                else:
                    a[r % 2, r // 2, :, lanes] = v

    def product(i, a, o, n):
        stride, taps, _ = LAYERS[i]
        acc = None
        for p in range(taps):
            left = a[pl.ds(o + p, n)] if stride == 1 else a[p % 2, pl.ds(o + p // 2, n)]
            _, w, depth = left.shape
            part = jnp.dot(left.reshape(n * w, depth), w_refs[i][p], preferred_element_type=F32)
            acc = part if acc is None else acc + part
        v = jnp.maximum(acc + b_refs[i][...], 0.0)
        return v.reshape(n, w, v.shape[-1])

    def inside(v, d):
        return jnp.where(has_block[d], v, 0.0)

    def first_step(i):
        j = turn(i, x)
        own_copy(j).wait()
        part_arrival(j).wait_recv()
        for d in range(2):
            @pl.when(has[d])
            def _():
                for c in range(2):
                    edge_arrival(d, c, j).wait_recv()
        s = s_refs[0]
        for c in range(2):
            at = pl.ds(PAD + c * col_half, col_half)
            s[0, 0, at, :] = xhalo[0, c, j].astype(F32)
            s[0, pl.ds(1, tile_rows), at, :] = ximg[c, j].astype(F32)
            s[0, tile_rows + 1, at, :] = xhalo[1, c, j].astype(F32)
        spread(0, range(tile_rows + 2), a_refs[0])
        for e in range(2):
            y_out[j, e] = product(0, a_refs[0], e * y_part, y_part).astype(BF16)
        edge = x // (RING - 1)
        y_leaves(j, edge)

        @pl.when(i >= half - RING)
        def _():
            y_leaves(turn(i - half + RING, x), 1 - edge)

    def forward(r):
        for d in range(2):
            y_arrival(r, d * (RING - 1), d).wait()

            @pl.when(has_block[d])
            def _():
                yh_copy(d, r).start()

    def second_step(r):
        a1, a2, a3 = a_refs[1], a_refs[2], a_refs[3].at[r]
        for src in range(RING):
            for e in range(2):
                if (src, e) not in ((0, 0), (RING - 1, 1)):
                    y_arrival(r, src, e).wait()
        for d in range(2):
            @pl.when(has_block[d])
            def _():
                block_arrival(y_halo, d, r, yh_send, yh_recv).wait_recv()
        own = RING * y_rows
        keep(1, y_halo[0, r].astype(F32), 0)
        for src in range(RING):
            for e in range(2):
                keep(1, y_in[r, src, e].astype(F32), 2 + src * y_rows + e * y_part)
        keep(1, y_halo[1, r].astype(F32), 2 + own)
        n = 3
        for o in range(0, own + 2, n):
            spread(1, range(o if o == 0 else o + 2, o + n + 2), a1)
            v = product(1, a1, o, n)
            if o == 0:
                keep(2, inside(v[:1], 0), 0)
                keep(2, v[1:], 1)
            elif o == own + 2 - n:
                keep(2, v[: n - 1], o)
                keep(2, inside(v[n - 1 :], 1), own + 1)
            else:
                keep(2, v, o)
            spread(2, range(o, o + n), a2)

        u_rows = own // 2
        depth = u_halo.shape[2]
        n = u_rows // 2
        for e in range(2):
            v = product(2, a2, e * n, n)
            u_out[e, r] = v.astype(BF16)
            keep(3, v, depth + e * n)
        for d in range(2):
            @pl.when(has_block[d])
            def _():
                u_copy(d, r).start()
        spread(3, range(depth, depth + u_rows), a3)

    def third_step(r):
        a3, a4, a5 = a_refs[3].at[r], a_refs[4], a_refs[5]
        depth = u_halo.shape[2]
        u_rows = RING * y_rows // 2
        n = (u_rows - 2) // 2
        for o in (depth, depth + n):
            keep(4, product(3, a3, o, n), o)
        spread(4, range(depth, depth + u_rows - 2), a4)
        for d in range(2):
            @pl.when(has_block[d])
            def _():
                block_arrival(u_halo, d, r, u_send, u_recv).wait_recv()
        for d, o in ((0, 0), (1, depth + u_rows)):
            keep(3, u_halo[d, r].astype(F32), o)
            spread(3, range(o, o + depth), a3)
        low = depth + u_rows - 2
        v = product(3, a3, 0, depth)
        keep(4, inside(v[: depth - 1], 0), 0)
        keep(4, v[depth - 1 :], depth - 1)
        v = product(3, a3, low, depth)
        keep(4, v[:1], low)
        keep(4, inside(v[1:], 1), low + 1)
        for o in (0, low):
            spread(4, range(o, o + depth), a4)
        f_rows = u_rows // 2
        v = product(4, a4, 0, f_rows + 2)
        keep(5, inside(v[:1], 0), 0)
        keep(5, v[1 : 1 + f_rows], 1)
        keep(5, inside(v[1 + f_rows :], 1), 1 + f_rows)
        spread(5, range(f_rows + 2), a5)
        v = product(5, a5, 0, f_rows)
        w = v.shape[1] // 2
        for t in range(f_rows):
            for c in range(2):
                f_out[t, c, r] = v[t, c * w : (c + 1) * w].astype(BF16)

    def ready(i):
        w_copy(i).wait()
        b_copy(i).wait()

    ready(0)
    pl.loop(0, half)(first_step)
    for i in range(half - RING, half):
        y_leaves(turn(i, x), 1 - x // (RING - 1))
    ready(1)
    ready(2)
    for r in range(per):
        forward(r)
    pl.loop(0, per)(second_step)
    for i in (3, 4, 5):
        ready(i)
    pl.loop(0, per)(third_step)

    for o in (2, 1, 3, 0):
        for c in range(2):
            if o:
                f_copy(o, c).start()
            else:
                @pl.when(k == c)
                def _():
                    f_stays().start()

                @pl.when(k != c)
                def _():
                    f_copy(0, c).start()

    for i in range(half):
        part_copy(turn(i, x)).wait_send()
        for d in range(2):
            @pl.when(has[d])
            def _():
                for c in range(2):
                    edge_copy(d, c, turn(i, (x + 2 * d - 1) % RING)).wait_send()
        if i % RING != RING - 1:
            for e in range(2):
                y_copy(turn(i, x), e).wait_send()
    for r in range(per):
        for d in range(2):
            @pl.when(has_block[d])
            def _():
                yh_copy(d, r).wait_send()
                u_copy(d, r).wait_send()
    for o in range(RING):
        for c in range(2):
            if o:
                f_copy(o, c).wait_send()
            else:
                @pl.when(k != c)
                def _():
                    f_copy(0, c).wait_send()
    for c in range(2):
        for src in range(RING):
            f_arrival(c, src).wait()
            for r in range(per):
                out_ref[c * half + r * RING + src, 0] = f_in[c, src, r]


def solution(mesh):
    row_len = mesh.shape["row"]

    def local_encoder(images, *params):
        n_img, rows, col_half, c_in = images.shape
        half = n_img // 2
        per = half // RING
        weights, biases = params[0::2], params[1::2]
        c_out = weights[0].shape[-1]
        args = [images]
        for w, b in zip(weights, biases):
            args += [w.reshape(w.shape[0], w.shape[1] * w.shape[2], c_out), b.reshape(1, c_out)]

        y_rows, u_rows, f_rows = rows // 2, RING * rows // 4, RING * rows // 8
        width = 2 * col_half
        depth1, depth3 = LAYERS[1][2], LAYERS[3][2]
        vmem, dma = pltpu.VMEM, pltpu.SemaphoreType.DMA
        scratch = [
            vmem((2, half, rows, col_half, c_in), BF16),
            vmem((2, n_img, col_half, c_in), BF16),
            vmem((2, 2, half, col_half, c_in), BF16),
            vmem((half, 2, y_rows // 2, width // 2, c_out), BF16),
            vmem((per, RING, 2, y_rows // 2, width // 2, c_out), BF16),
            vmem((2, per, depth1, width // 2, c_out), BF16),
            vmem((2, per, depth3, width // 4, c_out), BF16),
            vmem((2, per, depth3, width // 4, c_out), BF16),
            vmem((f_rows, 2, per, width // 16, c_out), BF16),
            vmem((2, RING, per, width // 16, c_out), BF16),
        ]
        scratch += [vmem(w.shape, BF16) for w in args[1::2]]
        scratch += [vmem((1, c_out), F32) for _ in biases]
        held, spans = [], (rows, RING * y_rows, RING * y_rows, u_rows, u_rows, f_rows)
        for i, (stride, taps, ext) in enumerate(LAYERS):
            chan = c_in if i == 0 else c_out
            total, w = spans[i] + 2 * ext, width // (1, 2, 2, 4, 4, 8)[i]
            shape = (total, w, taps * chan) if stride == 1 else (2, total // 2, w // 2, taps * chan)
            scratch.append(vmem((per,) + shape if i == 3 else shape, BF16))
            held.append(vmem((chan // LANES, total, w + 3 * PAD, LANES), F32))
        scratch += held
        scratch += [dma((6,)), dma((6,)), dma((half,)), dma((half,)), dma((half,)), dma((2,)), dma((2, 2, half)), dma((2, 2, half))]
        scratch += [dma((half, 2)), dma((per, RING, 2))] + [dma((2, per))] * 4 + [dma((RING, 2)), dma((2, RING))]

        any_spec = pl.BlockSpec(memory_space=pl.ANY)
        return pl.pallas_call(
            functools.partial(kernel, half, row_len),
            out_shape=jax.ShapeDtypeStruct((n_img, rows // 8, col_half // 8, c_out), BF16),
            in_specs=[any_spec] * len(args),
            out_specs=pl.BlockSpec(memory_space=pltpu.VMEM),
            scratch_shapes=scratch,
            compiler_params=pltpu.CompilerParams(collective_id=0, has_side_effects=True, vmem_limit_bytes=56 * 1024 * 1024),
            name="encoder",
        )(*args)

    tile_spec = P("batch", "row", "col", None)
    return jax.shard_map(local_encoder, mesh=mesh, in_specs=(tile_spec,) + (P(),) * 12, out_specs=tile_spec, check_vma=False)
```

```python
import functools

import jax
import jax.numpy as jnp
from jax import lax
from jax.experimental import pallas as pl
from jax.experimental.pallas import tpu as pltpu
from jax.sharding import PartitionSpec as P

MESH = pl.DeviceIdType.MESH
LANES = 128
PAD = 8
RING = 4

LAYERS = ((2, 4, 1), (1, 3, 2), (2, 4, 1), (1, 3, 4), (2, 4, 3), (1, 3, 1))
BF16, F32 = jnp.bfloat16, jnp.float32


def kernel(half, row_len, *refs):
    images_ref = refs[0]
    w_hbm, b_hbm = refs[1:13:2], refs[2:14:2]
    out_ref = refs[13]
    refs = refs[14:]
    ximg, xedge, xhalo, y_out, y_in, y_halo, u_out, u_halo, f_out, f_in = refs[:10]
    w_refs, b_all, a_refs, s_refs = refs[10:16], refs[16], refs[17:23], refs[23:29]
    (w_sem, b_sem, in_sem, part_send, load_sem, edge_send, edge_recv, y_send, y_recv, yh_send, yh_recv, u_send, u_recv, f_send, f_recv) = refs[29:]

    k = lax.axis_index("col")
    row = lax.axis_index("row")
    x = row % RING
    first = row - x
    per = half // RING
    has = (row > 0, row < row_len - 1)
    near = (jnp.maximum(row - 1, 0), jnp.minimum(row + 1, row_len - 1))
    has_block = (row >= RING, row < row_len - RING)
    near_block = (jnp.maximum(row - RING, 0), jnp.minimum(row + RING, row_len - 1))
    tile_rows, col_half = ximg.shape[2:4]
    y_part = y_out.shape[2]
    y_rows = 2 * y_part

    barrier = pltpu.get_barrier_semaphore()
    crosses = (jnp.logical_and(has[0], x == 0), jnp.logical_and(has[1], x == RING - 1))
    for d in range(2):
        @pl.when(crosses[d])
        def _():
            for c in range(2):
                pl.semaphore_signal(barrier, inc=1, device_id={"col": c, "row": near[d]}, device_id_type=MESH)

        @pl.when(has_block[d])
        def _():
            pl.semaphore_signal(barrier, inc=1, device_id={"row": near_block[d]}, device_id_type=MESH)
    for o in (2, 1, 3):
        for c in range(2):
            pl.semaphore_signal(barrier, inc=1, device_id={"col": c, "row": first + (x + o) % RING}, device_id_type=MESH)
    pl.semaphore_signal(barrier, inc=1, device_id={"col": 1 - k}, device_id_type=MESH)

    def turn(i, at):
        step, pair = i % RING, (i % RING) // 2
        offset = (1 - pair) * (2 + step) + pair * (3 - step)
        return (i // RING) * RING + (at + offset) % RING

    def settle(ref, sem):
        pltpu.make_async_copy(ref, ref, sem).wait()

    def edge_load(d):
        return pltpu.make_async_copy(images_ref.at[:, 0 if d == 0 else tile_rows - 1], xedge.at[d], load_sem.at[0])

    def own_copy(j):
        return pltpu.make_async_copy(images_ref.at[k * half + j], ximg.at[j, k], in_sem.at[j])

    def part_copy(j):
        return pltpu.make_async_remote_copy(
            images_ref.at[(1 - k) * half + j], ximg.at[j, k], part_send.at[0], in_sem.at[j],
            device_id={"col": 1 - k}, device_id_type=MESH,
        )

    def edge_copy(d, c, j):
        return pltpu.make_async_remote_copy(
            xedge.at[d, c * half + j], xhalo.at[1 - d, j, k], edge_send.at[d], edge_recv.at[1 - d, j],
            device_id={"col": c, "row": near[d]}, device_id_type=MESH,
        )

    def y_kind(at, e):
        place = 2 * at + e
        return 2 * ((place + 2 * RING - 2) // (2 * RING - 1)) - place // (2 * RING - 1)

    def y_copy(j, e):
        return pltpu.make_async_remote_copy(
            y_out.at[j, e], y_in.at[j // RING, 2 * x + e], y_send.at[0], y_recv.at[j // RING, y_kind(x, e)],
            device_id={"row": first + j % RING}, device_id_type=MESH,
        )

    def y_stays(j, e):
        return pltpu.make_async_copy(y_out.at[j, e], y_in.at[j // RING, 2 * x + e], y_recv.at[j // RING, y_kind(x, e)])

    def y_leaves(j, e):
        stays = j % RING == x

        @pl.when(stays)
        def _():
            y_stays(j, e).start()

        @pl.when(jnp.logical_not(stays))
        def _():
            y_copy(j, e).start()

    def block_copy(src, halo, d, r, send, recv):
        return pltpu.make_async_remote_copy(
            src, halo.at[1 - d, r], send.at[d], recv.at[1 - d, r], device_id={"row": near_block[d]}, device_id_type=MESH
        )

    def yh_copy(d, r):
        return block_copy(y_in.at[r, d * (2 * RING - 1)], y_halo, d, r, yh_send, yh_recv)

    def u_copy(d, r):
        return block_copy(u_out.at[d, r], u_halo, d, r, u_send, u_recv)

    def f_copy(o, c):
        to = (x + o) % RING
        return pltpu.make_async_remote_copy(
            f_out.at[2 * to + c], f_in.at[RING * k + x], f_send.at[0], f_recv.at[0],
            device_id={"col": c, "row": first + to}, device_id_type=MESH,
        )

    def f_stays():
        return pltpu.make_async_copy(f_out.at[2 * x + k], f_in.at[RING * k + x], f_recv.at[0])

    def w_copy(i):
        return pltpu.make_async_copy(w_hbm[i], w_refs[i], w_sem.at[i])

    def b_copy(i):
        return pltpu.make_async_copy(b_hbm[i], b_all.at[i], b_sem.at[0])

    for d in range(2):
        edge_load(d).start()
    for i in range(half):
        own_copy(turn(i, x)).start()
        if i == 0:
            w_copy(0).start()
    for i in range(6):
        b_copy(i).start()

    for (stride, _, _), s in zip(LAYERS, s_refs):
        w = s.shape[-2] - 3 * PAD
        edge = jnp.zeros(s.shape[:-2] + (PAD, LANES), F32)
        s[..., pl.ds(0, PAD), :] = edge
        s[..., pl.ds(PAD + w, PAD), :] = edge
    for d in range(2):
        @pl.when(jnp.logical_not(has[d]))
        def _():
            xhalo[d] = jnp.zeros(xhalo.shape[1:], BF16)

        @pl.when(jnp.logical_not(has_block[d]))
        def _():
            y_halo[d] = jnp.zeros(y_halo.shape[1:], BF16)
            u_halo[d] = jnp.zeros(u_halo.shape[1:], BF16)

    settle(xedge, load_sem.at[0])
    count = 2 * RING - 1
    for d in range(2):
        count = count + 2 * crosses[d].astype(jnp.int32) + has_block[d].astype(jnp.int32)
    pl.semaphore_wait(barrier, count)

    for i in range(half):
        part_copy(turn(i, x)).start()
        for d in range(2):
            @pl.when(has[d])
            def _():
                for c in range(2):
                    edge_copy(d, c, turn(i, (x + 2 * d - 1) % RING)).start()
    for i in range(1, 6):
        w_copy(i).start()

    def keep(i, v, r):
        s = s_refs[i]
        w = s.shape[-2] - 3 * PAD
        for h in range(v.shape[-1] // LANES):
            s[h, pl.ds(r, v.shape[0]), pl.ds(PAD, w), :] = v[:, :, h * LANES : (h + 1) * LANES]

    def spread(i, rows, a):
        stride, taps, _ = LAYERS[i]
        s = s_refs[i]
        w = (s.shape[-2] - 3 * PAD) // stride
        tiles = [(q, h) for q in range(taps) for h in range(s.shape[0])]
        for r in rows:
            for t in range(0, len(tiles), 2):
                pair = []
                for q, h in tiles[t : t + 2]:
                    at = pl.ds(PAD - 1 + q, w) if stride == 1 else pl.ds(PAD - 1 + q, w, stride=2)
                    pair.append(s[h, r, at, :])
                v = jnp.concatenate(pair, axis=-1).astype(BF16)
                lanes = pl.ds(t * LANES, 2 * LANES)
                if stride == 1:
                    a[r, :, lanes] = v
                else:
                    a[r % 2, r // 2, :, lanes] = v

    def product(i, a, o, n):
        stride, taps, _ = LAYERS[i]
        sums = [None, None]
        for p in range(taps):
            left = a[pl.ds(o + p, n)] if stride == 1 else a[p % 2, pl.ds(o + p // 2, n)]
            _, w, depth = left.shape
            left = left.reshape(n * w, depth)
            for b in range(0, depth, 2 * LANES):
                piece = jnp.dot(left[:, b : b + 2 * LANES], w_refs[i][p, pl.ds(b, 2 * LANES)], preferred_element_type=F32)
                at = int(i >= 4 and 2 * (p * depth + b) >= taps * depth)
                sums[at] = piece if sums[at] is None else sums[at] + piece
        acc = sums[0] if sums[1] is None else sums[0] + jnp.where(k >= 0, sums[1], 0.0)
        v = jnp.maximum(acc + b_all[i], 0.0)
        return v.reshape(n, w, v.shape[-1])

    def inside(v, d):
        return jnp.where(has_block[d], v, 0.0)

    def first_step(i):
        j = turn(i, x)
        settle(ximg.at[j], in_sem.at[j])
        for d in range(2):
            @pl.when(has[d])
            def _():
                settle(xhalo.at[d, j], edge_recv.at[d, j])
        s = s_refs[0]
        for c in range(2):
            at = pl.ds(PAD + c * col_half, col_half)
            s[0, 0, at, :] = xhalo[0, j, c].astype(F32)
            s[0, pl.ds(1, tile_rows), at, :] = ximg[j, c].astype(F32)
            s[0, tile_rows + 1, at, :] = xhalo[1, j, c].astype(F32)
        spread(0, range(tile_rows + 2), a_refs[0])
        for e in range(2):
            y_out[j, e] = product(0, a_refs[0], e * y_part, y_part).astype(BF16)
        edge = x // (RING - 1)
        y_leaves(j, edge)

        @pl.when(i >= half - RING)
        def _():
            y_leaves(turn(i - half + RING, x), 1 - edge)

    def forward(r):
        for d in range(2):
            settle(y_in.at[r, d * (2 * RING - 1)], y_recv.at[r, d])

            @pl.when(has_block[d])
            def _():
                yh_copy(d, r).start()

    def second_step(r):
        a1, a2, a3 = a_refs[1], a_refs[2], a_refs[3].at[r]
        own = RING * y_rows
        settle(y_in.at[r, pl.ds(1, 2 * RING - 2)], y_recv.at[r, 2])
        for place in range(2 * RING):
            keep(1, y_in[r, place].astype(F32), 2 + place * y_part)
        n = 3
        for o in range(n, own + 2 - n, n):
            spread(1, range(o if o == n else o + 2, o + n + 2), a1)
            keep(2, product(1, a1, o, n), o)
            spread(2, range(o, o + n), a2)
        for d in range(2):
            @pl.when(has_block[d])
            def _():
                settle(y_halo.at[d, r], yh_recv.at[d, r])
        keep(1, y_halo[0, r].astype(F32), 0)
        keep(1, y_halo[1, r].astype(F32), 2 + own)
        low = own + 2 - n
        spread(1, range(0, n), a1)
        v = product(1, a1, 0, n)
        spread(1, range(low + 2, own + 4), a1)
        u = product(1, a1, low, n)
        keep(2, inside(v[:1], 0), 0)
        keep(2, v[1:], 1)
        spread(2, range(n), a2)
        keep(2, u[: n - 1], low)
        keep(2, inside(u[n - 1 :], 1), own + 1)
        spread(2, range(low, low + n), a2)
        u_rows = own // 2
        depth = u_halo.shape[2]
        n = u_rows // 2
        for e in range(2):
            v = product(2, a2, e * n, n)
            u_out[e, r] = v.astype(BF16)
            keep(3, v, depth + e * n)
        for d in range(2):
            @pl.when(has_block[d])
            def _():
                u_copy(d, r).start()
        spread(3, range(depth, depth + u_rows), a3)

    def third_step(r):
        a3, a4, a5 = a_refs[3].at[r], a_refs[4], a_refs[5]
        depth = u_halo.shape[2]
        u_rows = RING * y_rows // 2
        n = (u_rows - 2) // 2
        for o in (depth, depth + n):
            keep(4, product(3, a3, o, n), o)
        spread(4, range(depth, depth + u_rows - 2), a4)
        for d in range(2):
            @pl.when(has_block[d])
            def _():
                settle(u_halo.at[d, r], u_recv.at[d, r])
        for d, o in ((0, 0), (1, depth + u_rows)):
            keep(3, u_halo[d, r].astype(F32), o)
            spread(3, range(o, o + depth), a3)
        low = depth + u_rows - 2
        v = product(3, a3, 0, depth)
        keep(4, inside(v[: depth - 1], 0), 0)
        keep(4, v[depth - 1 :], depth - 1)
        v = product(3, a3, low, depth)
        keep(4, v[:1], low)
        keep(4, inside(v[1:], 1), low + 1)
        for o in (0, low):
            spread(4, range(o, o + depth), a4)
        f_rows = u_rows // 2
        v = product(4, a4, 0, f_rows + 2)
        keep(5, inside(v[:1], 0), 0)
        keep(5, v[1 : 1 + f_rows], 1)
        keep(5, inside(v[1 + f_rows :], 1), 1 + f_rows)
        spread(5, range(f_rows + 2), a5)
        v = product(5, a5, 0, f_rows)
        w = v.shape[1] // 2
        for t in range(f_rows):
            for c in range(2):
                f_out[2 * t + c, r] = v[t, c * w : (c + 1) * w].astype(BF16)

    def ready(i):
        w_copy(i).wait()

    settle(b_all, b_sem.at[0])
    ready(0)
    pl.loop(0, half)(first_step)
    for i in range(half - RING, half):
        y_leaves(turn(i, x), 1 - x // (RING - 1))
    ready(1)
    ready(2)
    for r in range(per):
        forward(r)
    pl.loop(0, per)(second_step)
    for i in (3, 4, 5):
        ready(i)
    pl.loop(0, per)(third_step)

    for o in (2, 1, 3, 0):
        for c in range(2):
            if o:
                f_copy(o, c).start()
            else:
                @pl.when(k == c)
                def _():
                    f_stays().start()

                @pl.when(k != c)
                def _():
                    f_copy(0, c).start()

    settle(ximg.at[:, 0], part_send.at[0])
    settle(y_out.at[pl.ds(0, half - per)], y_send.at[0])
    for d in range(2):
        @pl.when(has[d])
        def _():
            settle(xedge.at[d], edge_send.at[d])

        @pl.when(has_block[d])
        def _():
            settle(y_halo.at[d], yh_send.at[d])
            settle(u_out.at[d], u_send.at[d])
    settle(f_out.at[pl.ds(0, 2 * RING - 1)], f_send.at[0])
    settle(f_in, f_recv.at[0])
    for c in range(2):
        for src in range(RING):
            for r in range(per):
                out_ref[c * half + r * RING + src, 0] = f_in[c * RING + src, r]


def solution(mesh):
    row_len = mesh.shape["row"]

    def local_encoder(images, *params):
        n_img, rows, col_half, c_in = images.shape
        half = n_img // 2
        per = half // RING
        weights, biases = params[0::2], params[1::2]
        c_out = weights[0].shape[-1]
        args = [images]
        for w, b in zip(weights, biases):
            args += [w.reshape(w.shape[0], w.shape[1] * w.shape[2], c_out), b.reshape(1, c_out)]
        args = [pltpu.with_memory_space_constraint(v, pltpu.HBM) for v in args]

        y_rows, u_rows, f_rows = rows // 2, RING * rows // 4, RING * rows // 8
        width = 2 * col_half
        depth1, depth3 = LAYERS[1][2], LAYERS[3][2]
        vmem, dma = pltpu.VMEM, pltpu.SemaphoreType.DMA
        scratch = [
            vmem((half, 2, rows, col_half, c_in), BF16),
            vmem((2, n_img, col_half, c_in), BF16),
            vmem((2, half, 2, col_half, c_in), BF16),
            vmem((half, 2, y_rows // 2, width // 2, c_out), BF16),
            vmem((per, 2 * RING, y_rows // 2, width // 2, c_out), BF16),
            vmem((2, per, depth1, width // 2, c_out), BF16),
            vmem((2, per, depth3, width // 4, c_out), BF16),
            vmem((2, per, depth3, width // 4, c_out), BF16),
            vmem((2 * f_rows, per, width // 16, c_out), BF16),
            vmem((2 * RING, per, width // 16, c_out), BF16),
        ]
        scratch += [vmem(w.shape, BF16) for w in args[1::2]]
        scratch += [vmem((6, 1, c_out), F32)]
        held, spans = [], (rows, RING * y_rows, RING * y_rows, u_rows, u_rows, f_rows)
        for i, (stride, taps, ext) in enumerate(LAYERS):
            chan = c_in if i == 0 else c_out
            total, w = spans[i] + 2 * ext, width // (1, 2, 2, 4, 4, 8)[i]
            shape = (total, w, taps * chan) if stride == 1 else (2, total // 2, w // 2, taps * chan)
            scratch.append(vmem((per,) + shape if i == 3 else shape, BF16))
            held.append(vmem((chan // LANES, total, w + 3 * PAD, LANES), F32))
        scratch += held
        scratch += [dma((6,)), dma((1,)), dma((half,)), dma((1,)), dma((1,)), dma((2,)), dma((2, half))]
        scratch += [dma((1,)), dma((per, 3))] + [dma((2,)), dma((2, per))] * 2 + [dma((1,)), dma((1,))]

        any_spec = pl.BlockSpec(memory_space=pl.ANY)
        return pl.pallas_call(
            functools.partial(kernel, half, row_len),
            out_shape=jax.ShapeDtypeStruct((n_img, rows // 8, col_half // 8, c_out), BF16),
            in_specs=[any_spec] * len(args),
            out_specs=pl.BlockSpec(memory_space=pltpu.VMEM),
            scratch_shapes=scratch,
            compiler_params=pltpu.CompilerParams(collective_id=0, has_side_effects=True, vmem_limit_bytes=53 * 1024 * 1024),
            name="encoder",
        )(*args)

    tile_spec = P("batch", "row", "col", None)
    return jax.shard_map(local_encoder, mesh=mesh, in_specs=(tile_spec,) + (P(),) * 12, out_specs=tile_spec, check_vma=False)
```

```python
import functools

import jax
import jax.numpy as jnp
from jax import lax
from jax.experimental import pallas as pl
from jax.experimental.pallas import tpu as pltpu
from jax.sharding import PartitionSpec as P

MESH = pl.DeviceIdType.MESH
LANES = 128
PAD = 8
RING = 4

LAYERS = ((2, 4, 1), (1, 3, 2), (2, 4, 1), (1, 3, 4), (2, 4, 3), (1, 3, 1))
BF16, F32 = jnp.bfloat16, jnp.float32


def kernel(half, row_len, *refs):
    images_ref = refs[0]
    w_hbm, b_hbm = refs[1:13:2], refs[2:14:2]
    out_ref = refs[13]
    refs = refs[14:]
    ximg, xedge, xhalo, y_out, y_in, y_halo, u_out, u_halo, f_out, f_in = refs[:10]
    w_refs, b_all, a_refs, s_refs = refs[10:16], refs[16], refs[17:23], refs[23:29]
    (w_sem, b_sem, in_sem, part_send, load_sem, edge_send, edge_recv, y_send, y_recv, yh_send, yh_recv, u_send, u_recv, f_send, f_recv) = refs[29:]

    k = lax.axis_index("col")
    row = lax.axis_index("row")
    x = row % RING
    first = row - x
    per = half // RING
    has = (row > 0, row < row_len - 1)
    near = (jnp.maximum(row - 1, 0), jnp.minimum(row + 1, row_len - 1))
    has_block = (row >= RING, row < row_len - RING)
    near_block = (jnp.maximum(row - RING, 0), jnp.minimum(row + RING, row_len - 1))
    tile_rows, col_half = ximg.shape[2:4]
    y_part = y_out.shape[2]
    y_rows = 2 * y_part

    barrier = pltpu.get_barrier_semaphore()
    crosses = (jnp.logical_and(has[0], x == 0), jnp.logical_and(has[1], x == RING - 1))
    for d in range(2):
        @pl.when(crosses[d])
        def _():
            for c in range(2):
                pl.semaphore_signal(barrier, inc=1, device_id={"col": c, "row": near[d]}, device_id_type=MESH)

        @pl.when(has_block[d])
        def _():
            pl.semaphore_signal(barrier, inc=1, device_id={"row": near_block[d]}, device_id_type=MESH)
    for o in (2, 1, 3):
        for c in range(2):
            pl.semaphore_signal(barrier, inc=1, device_id={"col": c, "row": first + (x + o) % RING}, device_id_type=MESH)
    pl.semaphore_signal(barrier, inc=1, device_id={"col": 1 - k}, device_id_type=MESH)

    def turn(i, at):
        step, pair = i % RING, (i % RING) // 2
        offset = (1 - pair) * (2 + step) + pair * (3 - step)
        return (i // RING) * RING + (at + offset) % RING

    def settle(ref, sem):
        pltpu.make_async_copy(ref, ref, sem).wait()

    def edge_load(d):
        return pltpu.make_async_copy(images_ref.at[:, 0 if d == 0 else tile_rows - 1], xedge.at[d], load_sem.at[0])

    def own_copy(j):
        return pltpu.make_async_copy(images_ref.at[k * half + j], ximg.at[j, k], in_sem.at[j])

    def part_copy(j):
        return pltpu.make_async_remote_copy(
            images_ref.at[(1 - k) * half + j], ximg.at[j, k], part_send.at[0], in_sem.at[j],
            device_id={"col": 1 - k}, device_id_type=MESH,
        )

    def edge_copy(d, c, j):
        return pltpu.make_async_remote_copy(
            xedge.at[d, c * half + j], xhalo.at[1 - d, j, k], edge_send.at[d], edge_recv.at[1 - d, j],
            device_id={"col": c, "row": near[d]}, device_id_type=MESH,
        )

    def y_kind(at, e):
        place = 2 * at + e
        return 2 * ((place + 2 * RING - 2) // (2 * RING - 1)) - place // (2 * RING - 1)

    def y_copy(j, e):
        return pltpu.make_async_remote_copy(
            y_out.at[j, e], y_in.at[j // RING, 2 * x + e], y_send.at[0], y_recv.at[j // RING, y_kind(x, e)],
            device_id={"row": first + j % RING}, device_id_type=MESH,
        )

    def y_stays(j, e):
        return pltpu.make_async_copy(y_out.at[j, e], y_in.at[j // RING, 2 * x + e], y_recv.at[j // RING, y_kind(x, e)])

    def y_leaves(j, e):
        stays = j % RING == x

        @pl.when(stays)
        def _():
            y_stays(j, e).start()

        @pl.when(jnp.logical_not(stays))
        def _():
            y_copy(j, e).start()

    def block_copy(src, halo, d, r, send, recv):
        return pltpu.make_async_remote_copy(
            src, halo.at[1 - d, r], send.at[d], recv.at[1 - d, r], device_id={"row": near_block[d]}, device_id_type=MESH
        )

    def yh_copy(d, r):
        return block_copy(y_in.at[r, d * (2 * RING - 1)], y_halo, d, r, yh_send, yh_recv)

    def u_copy(d, r, o):
        return pltpu.make_async_remote_copy(
            u_out.at[d, r, pl.ds(o, 2)], u_halo.at[1 - d, r, pl.ds(o, 2)], u_send.at[d], u_recv.at[1 - d, r],
            device_id={"row": near_block[d]}, device_id_type=MESH,
        )

    def f_copy(o, c):
        to = (x + o) % RING
        return pltpu.make_async_remote_copy(
            f_out.at[2 * to + c], f_in.at[RING * k + x], f_send.at[0], f_recv.at[0],
            device_id={"col": c, "row": first + to}, device_id_type=MESH,
        )

    def f_stays():
        return pltpu.make_async_copy(f_out.at[2 * x + k], f_in.at[RING * k + x], f_recv.at[0])

    def w_copy(i):
        return pltpu.make_async_copy(w_hbm[i], w_refs[i], w_sem.at[i])

    def b_copy(i):
        return pltpu.make_async_copy(b_hbm[i], b_all.at[i], b_sem.at[0])

    for d in range(2):
        edge_load(d).start()
    for i in range(half):
        own_copy(turn(i, x)).start()
        if i == 0:
            w_copy(0).start()
    for i in range(6):
        b_copy(i).start()

    for (stride, _, _), s in zip(LAYERS, s_refs):
        w = s.shape[-2] - 3 * PAD
        edge = jnp.zeros(s.shape[:-2] + (PAD, LANES), F32)
        s[..., pl.ds(0, PAD), :] = edge
        s[..., pl.ds(PAD + w, PAD), :] = edge
    for d in range(2):
        @pl.when(jnp.logical_not(has[d]))
        def _():
            xhalo[d] = jnp.zeros(xhalo.shape[1:], BF16)

        @pl.when(jnp.logical_not(has_block[d]))
        def _():
            y_halo[d] = jnp.zeros(y_halo.shape[1:], BF16)
            u_halo[d] = jnp.zeros(u_halo.shape[1:], BF16)

    settle(xedge, load_sem.at[0])
    count = 2 * RING - 1
    for d in range(2):
        count = count + 2 * crosses[d].astype(jnp.int32) + has_block[d].astype(jnp.int32)
    pl.semaphore_wait(barrier, count)

    for i in range(half):
        part_copy(turn(i, x)).start()
        for d in range(2):
            @pl.when(has[d])
            def _():
                for c in range(2):
                    edge_copy(d, c, turn(i, (x + 2 * d - 1) % RING)).start()
    for i in range(1, 6):
        w_copy(i).start()

    def keep(i, v, r):
        s = s_refs[i]
        w = s.shape[-2] - 3 * PAD
        for h in range(v.shape[-1] // LANES):
            s[h, pl.ds(r, v.shape[0]), pl.ds(PAD, w), :] = v[:, :, h * LANES : (h + 1) * LANES]

    def spread(i, rows, a):
        stride, taps, _ = LAYERS[i]
        s = s_refs[i]
        w = (s.shape[-2] - 3 * PAD) // stride
        tiles = [(q, h) for q in range(taps) for h in range(s.shape[0])]
        for r in rows:
            for t in range(0, len(tiles), 2):
                pair = []
                for q, h in tiles[t : t + 2]:
                    at = pl.ds(PAD - 1 + q, w) if stride == 1 else pl.ds(PAD - 1 + q, w, stride=2)
                    pair.append(s[h, r, at, :])
                v = jnp.concatenate(pair, axis=-1).astype(BF16)
                lanes = pl.ds(t * LANES, 2 * LANES)
                if stride == 1:
                    a[r, :, lanes] = v
                else:
                    a[r % 2, r // 2, :, lanes] = v

    def product(i, a, *spans):
        stride, taps, _ = LAYERS[i]
        sums = [None, None]
        for p in range(taps):
            parts = [a[pl.ds(o + p, n)] if stride == 1 else a[p % 2, pl.ds(o + p // 2, n)] for o, n in spans]
            left = parts[0] if len(parts) == 1 else jnp.concatenate(parts, axis=0)
            n, w, depth = left.shape
            left = left.reshape(n * w, depth)
            for b in range(0, depth, 2 * LANES):
                piece = jnp.dot(left[:, b : b + 2 * LANES], w_refs[i][p, pl.ds(b, 2 * LANES)], preferred_element_type=F32)
                at = int(i in (2, 4, 5) and 2 * (p * depth + b) >= taps * depth)
                sums[at] = piece if sums[at] is None else sums[at] + piece
        acc = sums[0] if sums[1] is None else sums[0] + jnp.where(k >= 0, sums[1], 0.0)
        v = jnp.maximum(acc + b_all[i], 0.0)
        return v.reshape(n, w, v.shape[-1])

    def inside(v, d):
        return jnp.where(has_block[d], v, 0.0)

    def first_step(i):
        j = turn(i, x)
        settle(ximg.at[j], in_sem.at[j])
        for d in range(2):
            @pl.when(has[d])
            def _():
                settle(xhalo.at[d, j], edge_recv.at[d, j])
        s = s_refs[0]
        for c in range(2):
            at = pl.ds(PAD + c * col_half, col_half)
            s[0, 0, at, :] = xhalo[0, j, c].astype(F32)
            s[0, pl.ds(1, tile_rows), at, :] = ximg[j, c].astype(F32)
            s[0, tile_rows + 1, at, :] = xhalo[1, j, c].astype(F32)
        spread(0, range(tile_rows + 2), a_refs[0])
        for e in range(2):
            y_out[j, e] = product(0, a_refs[0], (e * y_part, y_part)).astype(BF16)
        edge = x // (RING - 1)
        y_leaves(j, edge)

        @pl.when(i >= half - RING)
        def _():
            y_leaves(turn(i - half + RING, x), 1 - edge)

    def forward(r):
        for d in range(2):
            settle(y_in.at[r, d * (2 * RING - 1)], y_recv.at[r, d])

            @pl.when(has_block[d])
            def _():
                yh_copy(d, r).start()

    def second_step(r):
        a1, a2, a3 = a_refs[1], a_refs[2], a_refs[3].at[r]
        own = RING * y_rows
        settle(y_in.at[r, pl.ds(1, 2 * RING - 2)], y_recv.at[r, 2])
        for place in range(2 * RING):
            keep(1, y_in[r, place].astype(F32), 2 + place * y_part)
        n = 2
        m = (own - 6) // 2
        spread(1, range(4, 6), a1)
        for o, rows in ((4, m), (4 + m, m), (n, n), (own - n, n)):
            new = range(o, o + n) if o == n else range(o + n, o + n + rows)
            spread(1, new, a1)
            keep(2, product(1, a1, (o, rows)), o)
            spread(2, range(o, o + rows), a2)
        u_rows = own // 2
        depth = u_halo.shape[2]
        mid = product(2, a2, (2, u_rows - 4))
        u_out[0, r, pl.ds(2, depth - 2)] = mid[: depth - 2].astype(BF16)
        u_out[1, r, pl.ds(0, depth - 2)] = mid[depth - 2 :].astype(BF16)
        keep(3, mid, depth + 2)
        for d in range(2):
            @pl.when(has_block[d])
            def _():
                u_copy(d, r, 2 - 2 * d).start()

        for d in range(2):
            @pl.when(has_block[d])
            def _():
                settle(y_halo.at[d, r], yh_recv.at[d, r])
        keep(1, y_halo[0, r].astype(F32), 0)
        keep(1, y_halo[1, r].astype(F32), 2 + own)
        low = own + 2 - n
        spread(1, range(0, n), a1)
        v = product(1, a1, (0, n))
        spread(1, range(low + 2, own + 4), a1)
        u = product(1, a1, (low, n))
        keep(2, inside(v[:1], 0), 0)
        keep(2, v[1:], 1)
        spread(2, range(n), a2)
        keep(2, u[: n - 1], low)
        keep(2, inside(u[n - 1 :], 1), own + 1)
        spread(2, range(low, low + n), a2)
        rim = product(2, a2, (0, 2), (u_rows - 2, 2))
        u_out[0, r, pl.ds(0, 2)] = rim[:2].astype(BF16)
        u_out[1, r, pl.ds(depth - 2, 2)] = rim[2:].astype(BF16)
        for d in range(2):
            @pl.when(has_block[d])
            def _():
                u_copy(d, r, 2 * d).start()
        keep(3, rim[:2], depth)
        keep(3, rim[2:], depth + u_rows - 2)
        spread(3, range(depth, depth + u_rows), a3)

    def third_step(r):
        a3, a4, a5 = a_refs[3].at[r], a_refs[4], a_refs[5]
        depth = u_halo.shape[2]
        u_rows = RING * y_rows // 2
        n = (u_rows - 2) // 2
        for o in (depth, depth + n):
            keep(4, product(3, a3, (o, n)), o)
        spread(4, range(depth, depth + u_rows - 2), a4)
        for d in range(2):
            @pl.when(has_block[d])
            def _():
                settle(u_halo.at[d, r], u_recv.at[d, r])
        for d, o in ((0, 0), (1, depth + u_rows)):
            keep(3, u_halo[d, r].astype(F32), o)
            spread(3, range(o, o + depth), a3)
        low = depth + u_rows - 2
        v = product(3, a3, (0, depth))
        keep(4, inside(v[: depth - 1], 0), 0)
        keep(4, v[depth - 1 :], depth - 1)
        v = product(3, a3, (low, depth))
        keep(4, v[:1], low)
        keep(4, inside(v[1:], 1), low + 1)
        for o in (0, low):
            spread(4, range(o, o + depth), a4)
        f_rows = u_rows // 2
        v = product(4, a4, (0, f_rows + 2))
        keep(5, inside(v[:1], 0), 0)
        keep(5, v[1 : 1 + f_rows], 1)
        keep(5, inside(v[1 + f_rows :], 1), 1 + f_rows)
        spread(5, range(f_rows + 2), a5)
        v = product(5, a5, (0, f_rows))
        w = v.shape[1] // 2
        for t in range(f_rows):
            for c in range(2):
                f_out[2 * t + c, r] = v[t, c * w : (c + 1) * w].astype(BF16)

    def ready(i):
        w_copy(i).wait()

    settle(b_all, b_sem.at[0])
    ready(0)
    pl.loop(0, half)(first_step)
    for i in range(half - RING, half):
        y_leaves(turn(i, x), 1 - x // (RING - 1))
    ready(1)
    ready(2)
    for r in range(per):
        forward(r)
    pl.loop(0, per)(second_step)
    for i in (3, 4, 5):
        ready(i)
    pl.loop(0, per)(third_step)

    for o in (2, 1, 3, 0):
        for c in range(2):
            if o:
                f_copy(o, c).start()
            else:
                @pl.when(k == c)
                def _():
                    f_stays().start()

                @pl.when(k != c)
                def _():
                    f_copy(0, c).start()

    settle(ximg.at[:, 0], part_send.at[0])
    settle(y_out.at[pl.ds(0, half - per)], y_send.at[0])
    for d in range(2):
        @pl.when(has[d])
        def _():
            settle(xedge.at[d], edge_send.at[d])

        @pl.when(has_block[d])
        def _():
            settle(y_halo.at[d], yh_send.at[d])
            settle(u_out.at[d], u_send.at[d])
    settle(f_out.at[pl.ds(0, 2 * RING - 1)], f_send.at[0])
    settle(f_in, f_recv.at[0])
    for c in range(2):
        for src in range(RING):
            for r in range(per):
                out_ref[c * half + r * RING + src, 0] = f_in[c * RING + src, r]


def solution(mesh):
    row_len = mesh.shape["row"]

    def local_encoder(images, *params):
        n_img, rows, col_half, c_in = images.shape
        half = n_img // 2
        per = half // RING
        weights, biases = params[0::2], params[1::2]
        c_out = weights[0].shape[-1]
        args = [images]
        for w, b in zip(weights, biases):
            args += [w.reshape(w.shape[0], w.shape[1] * w.shape[2], c_out), b.reshape(1, c_out)]
        args = [pltpu.with_memory_space_constraint(v, pltpu.HBM) for v in args]

        y_rows, u_rows, f_rows = rows // 2, RING * rows // 4, RING * rows // 8
        width = 2 * col_half
        depth1, depth3 = LAYERS[1][2], LAYERS[3][2]
        vmem, dma = pltpu.VMEM, pltpu.SemaphoreType.DMA
        scratch = [
            vmem((half, 2, rows, col_half, c_in), BF16),
            vmem((2, n_img, col_half, c_in), BF16),
            vmem((2, half, 2, col_half, c_in), BF16),
            vmem((half, 2, y_rows // 2, width // 2, c_out), BF16),
            vmem((per, 2 * RING, y_rows // 2, width // 2, c_out), BF16),
            vmem((2, per, depth1, width // 2, c_out), BF16),
            vmem((2, per, depth3, width // 4, c_out), BF16),
            vmem((2, per, depth3, width // 4, c_out), BF16),
            vmem((2 * f_rows, per, width // 16, c_out), BF16),
            vmem((2 * RING, per, width // 16, c_out), BF16),
        ]
        scratch += [vmem(w.shape, BF16) for w in args[1::2]]
        scratch += [vmem((6, 1, c_out), F32)]
        held, spans = [], (rows, RING * y_rows, RING * y_rows, u_rows, u_rows, f_rows)
        for i, (stride, taps, ext) in enumerate(LAYERS):
            chan = c_in if i == 0 else c_out
            total, w = spans[i] + 2 * ext, width // (1, 2, 2, 4, 4, 8)[i]
            shape = (total, w, taps * chan) if stride == 1 else (2, total // 2, w // 2, taps * chan)
            scratch.append(vmem((per,) + shape if i == 3 else shape, BF16))
            held.append(vmem((chan // LANES, total, w + 3 * PAD, LANES), F32))
        scratch += held
        scratch += [dma((6,)), dma((1,)), dma((half,)), dma((1,)), dma((1,)), dma((2,)), dma((2, half))]
        scratch += [dma((1,)), dma((per, 3))] + [dma((2,)), dma((2, per))] * 2 + [dma((1,)), dma((1,))]

        any_spec = pl.BlockSpec(memory_space=pl.ANY)
        return pl.pallas_call(
            functools.partial(kernel, half, row_len),
            out_shape=jax.ShapeDtypeStruct((n_img, rows // 8, col_half // 8, c_out), BF16),
            in_specs=[any_spec] * len(args),
            out_specs=pl.BlockSpec(memory_space=pltpu.VMEM),
            scratch_shapes=scratch,
            compiler_params=pltpu.CompilerParams(collective_id=0, has_side_effects=True, vmem_limit_bytes=53 * 1024 * 1024),
            name="encoder",
        )(*args)

    tile_spec = P("batch", "row", "col", None)
    return jax.shard_map(local_encoder, mesh=mesh, in_specs=(tile_spec,) + (P(),) * 12, out_specs=tile_spec, check_vma=False)
```

```python
import functools

import jax
import jax.numpy as jnp
from jax import lax
from jax.experimental import pallas as pl
from jax.experimental.pallas import tpu as pltpu
from jax.sharding import PartitionSpec as P

MESH = pl.DeviceIdType.MESH
LANES = 128
PAD = 8
RING = 4

LAYERS = ((2, 4, 1), (1, 3, 2), (2, 4, 1), (1, 3, 4), (2, 4, 3), (1, 3, 1))
BF16, F32 = jnp.bfloat16, jnp.float32


def kernel(half, row_len, *refs):
    images_ref = refs[0]
    w_hbm, b_hbm = refs[1:13:2], refs[2:14:2]
    out_ref = refs[13]
    refs = refs[14:]
    ximg, xedge, xhalo, y_out, y_in, y_halo, u_out, u_halo, f_out, f_in = refs[:10]
    w_refs, b_all, a_refs, s_refs = refs[10:16], refs[16], refs[17:23], refs[23:29]
    (w_sem, b_sem, in_sem, part_send, load_sem, edge_send, edge_recv, y_send, y_recv, yh_send, yh_recv, u_send, u_recv, f_send, f_recv) = refs[29:]

    k = lax.axis_index("col")
    row = lax.axis_index("row")
    x = row % RING
    first = row - x
    per = half // RING
    has = (row > 0, row < row_len - 1)
    near = (jnp.maximum(row - 1, 0), jnp.minimum(row + 1, row_len - 1))
    has_block = (row >= RING, row < row_len - RING)
    near_block = (jnp.maximum(row - RING, 0), jnp.minimum(row + RING, row_len - 1))
    tile_rows, col_half = ximg.shape[2:4]
    y_part = y_out.shape[2]
    y_rows = 2 * y_part

    barrier = pltpu.get_barrier_semaphore()
    crosses = (jnp.logical_and(has[0], x == 0), jnp.logical_and(has[1], x == RING - 1))
    for d in range(2):
        @pl.when(crosses[d])
        def _():
            for c in range(2):
                pl.semaphore_signal(barrier, inc=1, device_id={"col": c, "row": near[d]}, device_id_type=MESH)

        @pl.when(has_block[d])
        def _():
            pl.semaphore_signal(barrier, inc=1, device_id={"row": near_block[d]}, device_id_type=MESH)
    for o in (2, 1, 3):
        for c in range(2):
            pl.semaphore_signal(barrier, inc=1, device_id={"col": c, "row": first + (x + o) % RING}, device_id_type=MESH)
    pl.semaphore_signal(barrier, inc=1, device_id={"col": 1 - k}, device_id_type=MESH)

    def turn(i, at):
        step, pair = i % RING, (i % RING) // 2
        offset = (1 - pair) * (2 + step) + pair * (3 - step)
        return (i // RING) * RING + (at + offset) % RING

    def settle(ref, sem):
        pltpu.make_async_copy(ref, ref, sem).wait()

    def edge_load(d):
        return pltpu.make_async_copy(images_ref.at[:, 0 if d == 0 else tile_rows - 1], xedge.at[d], load_sem.at[0])

    def own_copy(j):
        return pltpu.make_async_copy(images_ref.at[k * half + j], ximg.at[j, k], in_sem.at[j])

    def part_copy(j):
        return pltpu.make_async_remote_copy(
            images_ref.at[(1 - k) * half + j], ximg.at[j, k], part_send.at[0], in_sem.at[j],
            device_id={"col": 1 - k}, device_id_type=MESH,
        )

    def edge_copy(d, c, j):
        return pltpu.make_async_remote_copy(
            xedge.at[d, c * half + j], xhalo.at[1 - d, j, k], edge_send.at[d], edge_recv.at[1 - d, j],
            device_id={"col": c, "row": near[d]}, device_id_type=MESH,
        )

    def y_kind(at, e):
        place = 2 * at + e
        return 2 * ((place + 2 * RING - 2) // (2 * RING - 1)) - place // (2 * RING - 1)

    def y_copy(j, e):
        return pltpu.make_async_remote_copy(
            y_out.at[j, e], y_in.at[j // RING, 2 * x + e], y_send.at[0], y_recv.at[j // RING, y_kind(x, e)],
            device_id={"row": first + j % RING}, device_id_type=MESH,
        )

    def y_stays(j, e):
        return pltpu.make_async_copy(y_out.at[j, e], y_in.at[j // RING, 2 * x + e], y_recv.at[j // RING, y_kind(x, e)])

    def y_leaves(j, e):
        stays = j % RING == x

        @pl.when(stays)
        def _():
            y_stays(j, e).start()

        @pl.when(jnp.logical_not(stays))
        def _():
            y_copy(j, e).start()

    def block_copy(src, halo, d, r, send, recv):
        return pltpu.make_async_remote_copy(
            src, halo.at[1 - d, r], send.at[d], recv.at[1 - d, r], device_id={"row": near_block[d]}, device_id_type=MESH
        )

    def yh_copy(d, r):
        return block_copy(y_in.at[r, d * (2 * RING - 1)], y_halo, d, r, yh_send, yh_recv)

    def u_copy(d, r, o):
        return pltpu.make_async_remote_copy(
            u_out.at[d, r, pl.ds(o, 2)], u_halo.at[1 - d, r, pl.ds(o, 2)], u_send.at[d], u_recv.at[1 - d, r],
            device_id={"row": near_block[d]}, device_id_type=MESH,
        )

    def f_copy(o, c, r):
        to = (x + o) % RING
        return pltpu.make_async_remote_copy(
            f_out.at[2 * to + c, r], f_in.at[RING * k + x, r], f_send.at[0], f_recv.at[0],
            device_id={"col": c, "row": first + to}, device_id_type=MESH,
        )

    def f_stays(r):
        return pltpu.make_async_copy(f_out.at[2 * x + k, r], f_in.at[RING * k + x, r], f_recv.at[0])

    def w_copy(i):
        return pltpu.make_async_copy(w_hbm[i], w_refs[i], w_sem.at[i])

    def b_copy(i):
        return pltpu.make_async_copy(b_hbm[i], b_all.at[i], b_sem.at[0])

    for d in range(2):
        edge_load(d).start()
    for i in range(half):
        own_copy(turn(i, x)).start()
        if i == 0:
            w_copy(0).start()
    for i in range(6):
        b_copy(i).start()

    for (stride, _, _), s in zip(LAYERS, s_refs):
        w = s.shape[-2] - 3 * PAD
        edge = jnp.zeros(s.shape[:-2] + (PAD, LANES), F32)
        s[..., pl.ds(0, PAD), :] = edge
        s[..., pl.ds(PAD + w, PAD), :] = edge
    for d in range(2):
        @pl.when(jnp.logical_not(has[d]))
        def _():
            xhalo[d] = jnp.zeros(xhalo.shape[1:], BF16)

        @pl.when(jnp.logical_not(has_block[d]))
        def _():
            y_halo[d] = jnp.zeros(y_halo.shape[1:], BF16)
            u_halo[d] = jnp.zeros(u_halo.shape[1:], BF16)

    settle(xedge, load_sem.at[0])
    count = 2 * RING - 1
    for d in range(2):
        count = count + 2 * crosses[d].astype(jnp.int32) + has_block[d].astype(jnp.int32)
    pl.semaphore_wait(barrier, count)

    for i in range(half):
        part_copy(turn(i, x)).start()
        for d in range(2):
            @pl.when(has[d])
            def _():
                for c in range(2):
                    edge_copy(d, c, turn(i, (x + 2 * d - 1) % RING)).start()
    for i in range(1, 6):
        w_copy(i).start()

    def keep(i, v, r):
        s = s_refs[i]
        w = s.shape[-2] - 3 * PAD
        for h in range(v.shape[-1] // LANES):
            s[h, pl.ds(r, v.shape[0]), pl.ds(PAD, w), :] = v[:, :, h * LANES : (h + 1) * LANES]

    def spread(i, rows, a):
        stride, taps, _ = LAYERS[i]
        s = s_refs[i]
        w = (s.shape[-2] - 3 * PAD) // stride
        tiles = [(q, h) for q in range(taps) for h in range(s.shape[0])]
        for r in rows:
            for t in range(0, len(tiles), 2):
                pair = []
                for q, h in tiles[t : t + 2]:
                    at = pl.ds(PAD - 1 + q, w) if stride == 1 else pl.ds(PAD - 1 + q, w, stride=2)
                    pair.append(s[h, r, at, :])
                v = jnp.concatenate(pair, axis=-1).astype(BF16)
                lanes = pl.ds(t * LANES, 2 * LANES)
                if stride == 1:
                    a[r, :, lanes] = v
                else:
                    a[r % 2, r // 2, :, lanes] = v

    def product(i, a, *spans):
        stride, taps, _ = LAYERS[i]
        sums = [None, None]
        for p in range(taps):
            parts = [a[pl.ds(o + p, n)] if stride == 1 else a[p % 2, pl.ds(o + p // 2, n)] for o, n in spans]
            left = parts[0] if len(parts) == 1 else jnp.concatenate(parts, axis=0)
            n, w, depth = left.shape
            left = left.reshape(n * w, depth)
            for b in range(0, depth, 2 * LANES):
                piece = jnp.dot(left[:, b : b + 2 * LANES], w_refs[i][p, pl.ds(b, 2 * LANES)], preferred_element_type=F32)
                at = int(i in (2, 4, 5) and 2 * (p * depth + b) >= taps * depth)
                sums[at] = piece if sums[at] is None else sums[at] + piece
        acc = sums[0] if sums[1] is None else sums[0] + jnp.where(k >= 0, sums[1], 0.0)
        v = jnp.maximum(acc + b_all[i], 0.0)
        return v.reshape(n, w, v.shape[-1])

    def inside(v, d):
        return jnp.where(has_block[d], v, 0.0)

    def first_step(i):
        j = turn(i, x)
        settle(ximg.at[j], in_sem.at[j])
        for d in range(2):
            @pl.when(has[d])
            def _():
                settle(xhalo.at[d, j], edge_recv.at[d, j])
        s = s_refs[0]
        for c in range(2):
            at = pl.ds(PAD + c * col_half, col_half)
            s[0, 0, at, :] = xhalo[0, j, c].astype(F32)
            s[0, pl.ds(1, tile_rows), at, :] = ximg[j, c].astype(F32)
            s[0, tile_rows + 1, at, :] = xhalo[1, j, c].astype(F32)
        spread(0, range(tile_rows + 2), a_refs[0])
        for e in range(2):
            y_out[j, e] = product(0, a_refs[0], (e * y_part, y_part)).astype(BF16)
        edge = x // (RING - 1)
        y_leaves(j, edge)

        @pl.when(i >= half - RING)
        def _():
            y_leaves(turn(i - half + RING, x), 1 - edge)

    def forward(r):
        for d in range(2):
            settle(y_in.at[r, d * (2 * RING - 1)], y_recv.at[r, d])

            @pl.when(has_block[d])
            def _():
                yh_copy(d, r).start()

    def second_step(r):
        a1, a2, a3 = a_refs[1], a_refs[2], a_refs[3].at[r]
        own = RING * y_rows
        settle(y_in.at[r, pl.ds(1, 2 * RING - 2)], y_recv.at[r, 2])
        for place in range(2 * RING):
            keep(1, y_in[r, place].astype(F32), 2 + place * y_part)
        n = 2
        m = (own - 6) // 2
        spread(1, range(4, 6), a1)
        for o, rows in ((4, m), (4 + m, m), (n, n), (own - n, n)):
            new = range(o, o + n) if o == n else range(o + n, o + n + rows)
            spread(1, new, a1)
            keep(2, product(1, a1, (o, rows)), o)
            spread(2, range(o, o + rows), a2)
        u_rows = own // 2
        depth = u_halo.shape[2]
        mid = product(2, a2, (2, u_rows - 4))
        u_out[0, r, pl.ds(2, depth - 2)] = mid[: depth - 2].astype(BF16)
        u_out[1, r, pl.ds(0, depth - 2)] = mid[depth - 2 :].astype(BF16)
        keep(3, mid, depth + 2)
        for d in range(2):
            @pl.when(has_block[d])
            def _():
                u_copy(d, r, 2 - 2 * d).start()

        for d in range(2):
            @pl.when(has_block[d])
            def _():
                settle(y_halo.at[d, r], yh_recv.at[d, r])
        keep(1, y_halo[0, r].astype(F32), 0)
        keep(1, y_halo[1, r].astype(F32), 2 + own)
        low = own + 2 - n
        spread(1, range(0, n), a1)
        v = product(1, a1, (0, n))
        spread(1, range(low + 2, own + 4), a1)
        u = product(1, a1, (low, n))
        keep(2, inside(v[:1], 0), 0)
        keep(2, v[1:], 1)
        spread(2, range(n), a2)
        keep(2, u[: n - 1], low)
        keep(2, inside(u[n - 1 :], 1), own + 1)
        spread(2, range(low, low + n), a2)
        rim = product(2, a2, (0, 2), (u_rows - 2, 2))
        u_out[0, r, pl.ds(0, 2)] = rim[:2].astype(BF16)
        u_out[1, r, pl.ds(depth - 2, 2)] = rim[2:].astype(BF16)
        for d in range(2):
            @pl.when(has_block[d])
            def _():
                u_copy(d, r, 2 * d).start()
        keep(3, rim[:2], depth)
        keep(3, rim[2:], depth + u_rows - 2)
        spread(3, range(depth, depth + u_rows), a3)

    def third_step(r):
        a3, a4, a5 = a_refs[3].at[r], a_refs[4], a_refs[5]
        depth = u_halo.shape[2]
        u_rows = RING * y_rows // 2
        n = (u_rows - 2) // 2
        for o in (depth, depth + n):
            keep(4, product(3, a3, (o, n)), o)
        spread(4, range(depth, depth + u_rows - 2), a4)
        for d in range(2):
            @pl.when(has_block[d])
            def _():
                settle(u_halo.at[d, r], u_recv.at[d, r])
        for d, o in ((0, 0), (1, depth + u_rows)):
            keep(3, u_halo[d, r].astype(F32), o)
            spread(3, range(o, o + depth), a3)
        low = depth + u_rows - 2
        v = product(3, a3, (0, depth))
        keep(4, inside(v[: depth - 1], 0), 0)
        keep(4, v[depth - 1 :], depth - 1)
        v = product(3, a3, (low, depth))
        keep(4, v[:1], low)
        keep(4, inside(v[1:], 1), low + 1)
        for o in (0, low):
            spread(4, range(o, o + depth), a4)
        f_rows = u_rows // 2
        v = product(4, a4, (0, f_rows + 2))
        keep(5, inside(v[:1], 0), 0)
        keep(5, v[1 : 1 + f_rows], 1)
        keep(5, inside(v[1 + f_rows :], 1), 1 + f_rows)
        spread(5, range(f_rows + 2), a5)
        v = product(5, a5, (0, f_rows))
        w = v.shape[1] // 2
        for t in range(f_rows):
            for c in range(2):
                f_out[2 * t + c, r] = v[t, c * w : (c + 1) * w].astype(BF16)

        for o in (2, 1, 3, 0):
            for c in range(2):
                if o:
                    f_copy(o, c, r).start()
                else:
                    @pl.when(k == c)
                    def _():
                        f_stays(r).start()

                    @pl.when(k != c)
                    def _():
                        f_copy(0, c, r).start()

    def ready(i):
        w_copy(i).wait()

    settle(b_all, b_sem.at[0])
    ready(0)
    pl.loop(0, half)(first_step)
    for i in range(half - RING, half):
        y_leaves(turn(i, x), 1 - x // (RING - 1))
    ready(1)
    ready(2)
    for r in range(per):
        forward(r)
    pl.loop(0, per)(second_step)
    for i in (3, 4, 5):
        ready(i)
    pl.loop(0, per)(third_step)

    settle(ximg.at[:, 0], part_send.at[0])
    settle(y_out.at[pl.ds(0, half - per)], y_send.at[0])
    for d in range(2):
        @pl.when(has[d])
        def _():
            settle(xedge.at[d], edge_send.at[d])

        @pl.when(has_block[d])
        def _():
            settle(y_halo.at[d], yh_send.at[d])
            settle(u_out.at[d], u_send.at[d])
    settle(f_out.at[pl.ds(0, 2 * RING - 1)], f_send.at[0])
    settle(f_in, f_recv.at[0])
    for c in range(2):
        for src in range(RING):
            for r in range(per):
                out_ref[c * half + r * RING + src, 0] = f_in[c * RING + src, r]


def solution(mesh):
    row_len = mesh.shape["row"]

    def local_encoder(images, *params):
        n_img, rows, col_half, c_in = images.shape
        half = n_img // 2
        per = half // RING
        weights, biases = params[0::2], params[1::2]
        c_out = weights[0].shape[-1]
        args = [images]
        for w, b in zip(weights, biases):
            args += [w.reshape(w.shape[0], w.shape[1] * w.shape[2], c_out), b.reshape(1, c_out)]
        args = [pltpu.with_memory_space_constraint(v, pltpu.HBM) for v in args]

        y_rows, u_rows, f_rows = rows // 2, RING * rows // 4, RING * rows // 8
        width = 2 * col_half
        depth1, depth3 = LAYERS[1][2], LAYERS[3][2]
        vmem, dma = pltpu.VMEM, pltpu.SemaphoreType.DMA
        scratch = [
            vmem((half, 2, rows, col_half, c_in), BF16),
            vmem((2, n_img, col_half, c_in), BF16),
            vmem((2, half, 2, col_half, c_in), BF16),
            vmem((half, 2, y_rows // 2, width // 2, c_out), BF16),
            vmem((per, 2 * RING, y_rows // 2, width // 2, c_out), BF16),
            vmem((2, per, depth1, width // 2, c_out), BF16),
            vmem((2, per, depth3, width // 4, c_out), BF16),
            vmem((2, per, depth3, width // 4, c_out), BF16),
            vmem((2 * f_rows, per, width // 16, c_out), BF16),
            vmem((2 * RING, per, width // 16, c_out), BF16),
        ]
        scratch += [vmem(w.shape, BF16) for w in args[1::2]]
        scratch += [vmem((6, 1, c_out), F32)]
        held, spans = [], (rows, RING * y_rows, RING * y_rows, u_rows, u_rows, f_rows)
        for i, (stride, taps, ext) in enumerate(LAYERS):
            chan = c_in if i == 0 else c_out
            total, w = spans[i] + 2 * ext, width // (1, 2, 2, 4, 4, 8)[i]
            shape = (total, w, taps * chan) if stride == 1 else (2, total // 2, w // 2, taps * chan)
            scratch.append(vmem((per,) + shape if i == 3 else shape, BF16))
            held.append(vmem((chan // LANES, total, w + 3 * PAD, LANES), F32))
        scratch += held
        scratch += [dma((6,)), dma((1,)), dma((half,)), dma((1,)), dma((1,)), dma((2,)), dma((2, half))]
        scratch += [dma((1,)), dma((per, 3))] + [dma((2,)), dma((2, per))] * 2 + [dma((1,)), dma((1,))]

        any_spec = pl.BlockSpec(memory_space=pl.ANY)
        return pl.pallas_call(
            functools.partial(kernel, half, row_len),
            out_shape=jax.ShapeDtypeStruct((n_img, rows // 8, col_half // 8, c_out), BF16),
            in_specs=[any_spec] * len(args),
            out_specs=pl.BlockSpec(memory_space=pltpu.VMEM),
            scratch_shapes=scratch,
            compiler_params=pltpu.CompilerParams(collective_id=0, has_side_effects=True, vmem_limit_bytes=53 * 1024 * 1024),
            name="encoder",
        )(*args)

    tile_spec = P("batch", "row", "col", None)
    return jax.shard_map(local_encoder, mesh=mesh, in_specs=(tile_spec,) + (P(),) * 12, out_specs=tile_spec, check_vma=False)
```
